256 devices in a mesh: space: 32 (over z, x_hi, core), bead: 8 (over y, x_lo).
Axes of the slice: x: 4 (x_hi: 2, x_lo: 2; x = x_hi * 2 + x_lo), y: 4, z: 8, core: 2. Of those that a mesh axis runs over, the one named last changes fastest.
Arguments:
- positions: float32 [32, 3, 131072], P('bead', None, 'space'), may hold values from -5 to 5
- momenta: float32 [32, 3, 131072], P('bead', None, 'space'), may hold values from -12 to 12
- masses: float32 [131072], P('space'), may hold values from 1 to 16
- strengths: float32 [131072], P('space'), may hold values from 0.5 to 2
- bond_ends: int32 [2, 131072], P(None, 'space'), may hold values from 0 to 127
- angle_ends: int32 [3, 65536], P(None, 'space'), may hold values from 0 to 127
- neighbour_tiles: int32 [3, 1024], P(None, 'space'), may hold values from 0 to 1023, as said below
Outputs:
- new_positions: float32 [32, 3, 131072], P('bead', None, 'space')
- new_momenta: float32 [32, 3, 131072], P('bead', None, 'space')
The draws below stay inside these ranges and needn't reach their ends.
Inputs may be any that keep to these rules, and one draw needn't show every extreme that they name: `bond_ends`: entry [e, b] is the place within tile b // 128 of end e of bond b. `angle_ends`: entry [e, b] is the place within tile b // 64 of atom e of angle b. `neighbour_tiles`: column t names 3 different tiles, each within 2 tiles of t, counting around the ends (tile 1024 - 1 lies next to tile 0).
All inputs are finite; a program needn't handle non-finite values.
Results may differ from the reference program's by a relative error of at most 0.0003.
Values sent between devices are 32-bit elements; how exact they have to be, the bound alone decides.
A program may use at most 64 MiB of HBM per device.

```python
import math
import jax
import jax.numpy as jnp
import numpy as np
from jax import lax

BEADS = 32
KEPT = 4
SUBS = 3
TILE = 128
GT = 2
NBR = 3
BPT = 128
APT = 64
NA = 131072
NT_ALL = 1024
NBONDS = 131072
NANGLES = 65536


spring_freq = 80.0


def bead_modes(number):
    within = np.arange(number)
    result = np.zeros((number, number))
    for column in range(number):
        if column == 0:
            result[:, column] = 1.0 / math.sqrt(number)
        elif 2 * column < number:
            result[:, column] = math.sqrt(2.0 / number) * np.cos(2 * np.pi * within * column / number)
        elif 2 * column == number:
            result[:, column] = (-1.0) ** within / math.sqrt(number)
        else:
            result[:, column] = math.sqrt(2.0 / number) * np.sin(2 * np.pi * within * column / number)
    return result


def draw_positions(key, part):
    table = jnp.asarray(bead_modes(BEADS), jnp.float32)
    freqs = 2.0 * spring_freq * np.sin(np.pi * np.arange(BEADS) / BEADS)
    safe = np.where(freqs > 0, freqs, 1.0)
    amps = jnp.asarray(np.where(freqs > 0, 1.0 / safe, 0.0), jnp.float32)
    centre_key = jax.random.fold_in(key, 11)
    mode_key = jax.random.fold_in(key, 23)
    centre = jax.random.truncated_normal(centre_key, -4.0, 4.0, (1, 3, NA), jnp.float32)
    modes = jax.random.uniform(mode_key, (BEADS, 3, NA), jnp.float32, -1.0, 1.0) * amps[:, None, None]
    spread = jnp.einsum('jk,kcl->jcl', table, modes, precision=lax.Precision.HIGHEST)
    return (centre + spread).astype(jnp.float32)


def draw_neighbour_tiles(key, part):
    width = 2 * GT + 1
    scores = jax.random.randint(key, (NT_ALL, width), 0, 2 ** 20) * width + jnp.arange(width, dtype=jnp.int32)[None, :]
    ranking = jnp.argsort(scores, axis=1, stable=True)[:, :NBR].astype(jnp.int32) - GT
    chosen = jnp.arange(NT_ALL, dtype=jnp.int32)[:, None] + ranking
    return jnp.mod(chosen, NT_ALL).T.astype(jnp.int32)


def place_ends(array, key, low, largest):
    place = [jax.random.randint(jax.random.fold_in(key, axis), (), 0, length) for axis, length in enumerate(array.shape)]
    longest = array.shape.index(max(array.shape))
    beside = place[:longest] + [(place[longest] + 1) % array.shape[longest]] + place[longest + 1:]
    return array.at[tuple(place)].set(low).at[tuple(beside)].set(largest)


def levels(stream_key, extent, pieces, least, high):
    def one(dim, blocks):
        heights = jax.random.uniform(jax.random.fold_in(jax.random.fold_in(stream_key, 6), dim), (blocks,), jnp.float32, least / len(pieces), high / len(pieces))
        return jnp.repeat(jnp.exp(heights), extent[dim] // blocks).reshape((-1,) + (1,) * (len(extent) - dim - 1))

    level = one(*pieces[0])
    for cut in pieces[1:]:
        level = level * one(*cut)
    return level


def noise(rng, extent, scale, limit, cuts=(), kind=jnp.bfloat16):
    entries = jax.random.normal(rng, extent, jnp.float32) * scale
    if len(cuts) > 0:
        entries = levels(rng, extent, cuts, -0.22, 0.18) * entries
    return jnp.clip(entries, min=-limit, max=limit).astype(kind)


def setup_inputs(seed: int = 0) -> dict:
    streams_of = jax.random.split(jax.random.key(seed), 8)
    return {
        "positions": draw_positions(jax.random.fold_in(streams_of[7], 71), 0),
        "momenta": noise(streams_of[1], (BEADS, 3, NA), 2.0, 12.0, ((0, 8), (2, 32)), jnp.float32),
        "masses": jnp.clip(jnp.exp(math.log(16.0) - 2.7725887 * jax.random.uniform(streams_of[2], (NA,), jnp.float32) ** levels(streams_of[2], (NA,), ((0, 32),), -0.2, 0.2)), 1.0, 16.0),
        "strengths": jnp.clip(jnp.exp(math.log(2.0) - 1.3862944 * jax.random.uniform(streams_of[3], (NA,), jnp.float32) ** levels(streams_of[3], (NA,), ((0, 32),), -0.2, 0.2)), 0.5, 2.0),
        "bond_ends": place_ends(jax.random.randint(streams_of[4], (2, NBONDS), 0, TILE), jax.random.fold_in(streams_of[4], 1), 0, TILE - 1).astype(jnp.int32),
        "angle_ends": place_ends(jax.random.randint(streams_of[5], (3, NANGLES), 0, TILE), jax.random.fold_in(streams_of[5], 1), 0, TILE - 1).astype(jnp.int32),
        "neighbour_tiles": draw_neighbour_tiles(jax.random.fold_in(streams_of[7], 71), 0),
    }


time_step = 0.3
spring_freq = 80.0
bond_stiff = 0.2
bond_rest = 1.0
angle_stiff = 0.1
angle_rest = 0.5
range_sq = 4.0
HIGH = lax.Precision.HIGHEST

def mode_table(number):
    within = np.arange(number)
    result = np.zeros((number, number))
    for column in range(number):
        if column == 0:
            result[:, column] = 1.0 / math.sqrt(number)
        elif 2 * column < number:
            result[:, column] = math.sqrt(2.0 / number) * np.cos(2 * np.pi * within * column / number)
        elif 2 * column == number:
            result[:, column] = (-1.0) ** within / math.sqrt(number)
        else:
            result[:, column] = math.sqrt(2.0 / number) * np.sin(2 * np.pi * within * column / number)
    return result

def contract_table(number, kept):
    larger = mode_table(number)
    smaller = mode_table(kept)
    chosen = [column if 2 * column <= kept else number - kept + column for column in range(kept)]
    return math.sqrt(kept / number) * smaller @ larger[:, chosen].T

def orbit_tables(number, interval):
    freqs = 2.0 * spring_freq * np.sin(np.pi * np.arange(number) / number)
    cosine = np.cos(freqs * interval)
    safe = np.where(freqs > 0, freqs, 1.0)
    gains = np.where(freqs > 0, np.sin(freqs * interval) / safe, interval)
    drags = freqs * np.sin(freqs * interval)
    return (cosine, gains, drags)

def propagate(current, moment, masses, modes_table, cosine, gains, drags):
    modes_pos = jnp.einsum('jk,jcl->kcl', modes_table, current, precision=HIGH)
    modes_mom = jnp.einsum('jk,jcl->kcl', modes_table, moment, precision=HIGH)
    moved_pos = cosine[:, None, None] * modes_pos + gains[:, None, None] * modes_mom / masses
    moved_mom = cosine[:, None, None] * modes_mom - drags[:, None, None] * masses * modes_pos
    return (jnp.einsum('jk,kcl->jcl', modes_table, moved_pos, precision=HIGH), jnp.einsum('jk,kcl->jcl', modes_table, moved_mom, precision=HIGH))

def pair_block(own_tiles, nearby, own_scale, nearby_scale):
    own_sq = lax.optimization_barrier(jnp.sum(own_tiles * own_tiles, axis=1))
    nearby_sq = lax.optimization_barrier(jnp.sum(nearby * nearby, axis=1))
    inner = jnp.einsum('cxta,cxtn->ctan', own_tiles, nearby, precision=HIGH)
    distance = own_sq[..., None] + nearby_sq[:, :, None, :] - 2.0 * inner
    weight = jnp.exp(-distance / range_sq) * nearby_scale[None, :, None, :]
    weight_sum = lax.optimization_barrier(jnp.sum(weight, axis=3))
    pulled = jnp.einsum('ctan,cxtn->cxta', weight, nearby, precision=HIGH)
    return 2.0 / range_sq * own_scale[None, None] * (own_tiles * weight_sum[:, None] - pulled)

def tile_forces(extended, scale_ext, own_first, tile_count, local_nbr):
    kept = extended.shape[0]
    tiled = extended.reshape(kept, 3, -1, TILE)
    scale_tiles = scale_ext.reshape(-1, TILE)
    group_size = math.gcd(tile_count, 8)
    rounds = tile_count // group_size
    width = local_nbr.shape[1]

    def one_group(offset):
        own_tiles = lax.dynamic_slice_in_dim(tiled, own_first + offset, group_size, 2)
        own_scale = lax.dynamic_slice_in_dim(scale_tiles, own_first + offset, group_size, 0)
        chosen = lax.dynamic_slice_in_dim(local_nbr, offset, group_size, 0).reshape(-1)
        nearby = jnp.take(tiled, chosen, axis=2).reshape(kept, 3, group_size, width * TILE)
        nearby_scale = jnp.take(scale_tiles, chosen, axis=0).reshape(group_size, width * TILE)
        return pair_block(own_tiles, nearby, own_scale, nearby_scale)
    offsets = jnp.arange(rounds, dtype=jnp.int32) * group_size
    result = lax.map(one_group, offsets)
    return jnp.moveaxis(result, 0, 2).reshape(kept, 3, tile_count * TILE)

def bonded(current, bond_ends, angle_ends):
    bond_base = jnp.arange(bond_ends.shape[1], dtype=jnp.int32) // BPT * TILE
    one_end = bond_base + bond_ends[0]
    other_end = bond_base + bond_ends[1]
    stretch = current[:, :, one_end] - current[:, :, other_end]
    factor = bond_stiff * (lax.optimization_barrier(jnp.sum(stretch * stretch, axis=1, keepdims=True)) - bond_rest)
    push = -factor * stretch
    forces = jnp.zeros_like(current).at[:, :, one_end].add(push).at[:, :, other_end].add(-push)
    angle_base = jnp.arange(angle_ends.shape[1], dtype=jnp.int32) // APT * TILE
    outer_one = angle_base + angle_ends[0]
    centre = angle_base + angle_ends[1]
    outer_two = angle_base + angle_ends[2]
    to_first = current[:, :, outer_one] - current[:, :, centre]
    to_last = current[:, :, outer_two] - current[:, :, centre]
    factor = angle_stiff * (lax.optimization_barrier(jnp.sum(to_first * to_last, axis=1, keepdims=True)) - angle_rest)
    forces = forces.at[:, :, outer_one].add(-factor * to_last)
    forces = forces.at[:, :, outer_two].add(-factor * to_first)
    forces = forces.at[:, :, centre].add(factor * (to_first + to_last))
    return forces

def reference(positions, momenta, masses, strengths, bond_ends, angle_ends, neighbour_tiles):
    interval = time_step / SUBS
    modes_table = jnp.asarray(mode_table(BEADS), jnp.float32)
    contract = jnp.asarray(contract_table(BEADS, KEPT), jnp.float32)
    expand = BEADS / KEPT * contract.T
    cos_np, gain_np, drag_np = orbit_tables(BEADS, interval)
    cosine = jnp.asarray(cos_np, jnp.float32)
    gains = jnp.asarray(gain_np, jnp.float32)
    drags = jnp.asarray(drag_np, jnp.float32)

    def nonbonded(current):
        contracted = jnp.einsum('kj,jcl->kcl', contract, current, precision=HIGH)
        nearby = tile_forces(contracted, strengths, 0, NT_ALL, neighbour_tiles.T.astype(jnp.int32))
        return jnp.einsum('jk,kcl->jcl', expand, nearby, precision=HIGH)
    current = positions
    moment = momenta + 0.5 * time_step * nonbonded(current)
    pushed = bonded(current, bond_ends, angle_ends)
    for substep in range(SUBS):
        moment = moment + 0.5 * interval * pushed
        current, moment = propagate(current, moment, masses, modes_table, cosine, gains, drags)
        pushed = bonded(current, bond_ends, angle_ends)
        moment = moment + 0.5 * interval * pushed
    moment = moment + 0.5 * time_step * nonbonded(current)
    return (current, moment)
```

```python
import functools
import math

import jax
import jax.numpy as jnp
import ml_dtypes
import numpy as np
from jax import lax
from jax.experimental import pallas as pl
from jax.experimental.pallas import tpu as pltpu
from jax.sharding import PartitionSpec as P

BEADS = 32
KEPT = 4
SUBS = 3
TILE = 128
GT = 2
NBR = 3
BPT = 128
APT = 64

time_step = 0.3
spring_freq = 80.0
bond_stiff = 0.2
bond_rest = 1.0
angle_stiff = 0.1
angle_rest = 0.5
range_sq = 4.0

F32 = jnp.float32
BF16 = jnp.bfloat16
MESH = pl.DeviceIdType.MESH


def mode_table(number):
    within = np.arange(number)
    result = np.zeros((number, number))
    for column in range(number):
        if column == 0:
            result[:, column] = 1.0 / math.sqrt(number)
        elif 2 * column < number:
            result[:, column] = math.sqrt(2.0 / number) * np.cos(2 * np.pi * within * column / number)
        elif 2 * column == number:
            result[:, column] = (-1.0) ** within / math.sqrt(number)
        else:
            result[:, column] = math.sqrt(2.0 / number) * np.sin(2 * np.pi * within * column / number)
    return result


def contract_table(number, kept):
    larger = mode_table(number)
    smaller = mode_table(kept)
    chosen = [column if 2 * column <= kept else number - kept + column for column in range(kept)]
    return math.sqrt(kept / number) * smaller @ larger[:, chosen].T


def halves(table):
    high = table.astype(ml_dtypes.bfloat16)
    low = (table - high.astype(np.float64)).astype(ml_dtypes.bfloat16)
    return high, low


def three_products(table):
    high, low = halves(table)
    return np.concatenate([high, low, high], axis=1)


def constant_table():
    modes = mode_table(BEADS)
    interval = time_step / SUBS
    freqs = 2.0 * spring_freq * np.sin(np.pi * np.arange(BEADS) / BEADS)
    safe = np.where(freqs > 0, freqs, 1.0)
    cosine = np.cos(freqs * interval)
    gains = np.where(freqs > 0, np.sin(freqs * interval) / safe, interval)
    drags = freqs * np.sin(freqs * interval)
    keep = (modes * cosine) @ modes.T
    gain = (modes * gains) @ modes.T
    drag = -(modes * drags) @ modes.T
    free = np.block([[keep, gain], [drag, keep]])
    contract = contract_table(BEADS, KEPT)
    narrow = np.zeros((16, 3 * BEADS))
    for k in range(KEPT):
        for c in range(3):
            narrow[3 * k + c, c * BEADS : (c + 1) * BEADS] = contract[k]
    expand = BEADS / KEPT * contract.T
    wide = np.zeros((3 * BEADS, 16))
    for k in range(KEPT):
        for c in range(3):
            wide[c * BEADS : (c + 1) * BEADS, 3 * k + c] = expand[:, k]
    wide *= 0.5 * time_step * 2.0 / range_sq
    table = np.zeros((64 + 16 + 96, 384), ml_dtypes.bfloat16)
    table[:64, :192] = three_products(free)
    table[64:80, :288] = three_products(narrow)
    table[80:176, :48] = three_products(wide)
    return table


def split2(x):
    high = x.astype(BF16)
    return high, (x - high.astype(F32)).astype(BF16)


def split3(x):
    high = x.astype(BF16)
    rest = x - high.astype(F32)
    middle = rest.astype(BF16)
    return high, middle, (rest - middle.astype(F32)).astype(BF16)


def mm(a, b):
    return jnp.dot(a, b, preferred_element_type=F32)


def lanes(x, t):
    return x[:, t * TILE : (t + 1) * TILE]


def kernel(
    spaces,
    beads,
    q_in,
    p_in,
    mass_in,
    strength_in,
    bond_in,
    angle_in,
    nbr_in,
    const_in,
    q_out,
    p_out,
    q_stage,
    p_stage,
    q_all,
    p_all,
    q_done,
    p_done,
    mass_v,
    strength_v,
    bond_v,
    angle_v,
    nbr_s,
    const_v,
    pick,
    drop,
    ext,
    a_side,
    g_side,
    local_sem,
    send_sem,
    recv_sem,
    own_sem,
    halo_send,
    halo_recv,
):
    space = lax.axis_index("space")
    me = lax.axis_index("bead")
    slab = q_in.shape[2]
    own = slab // beads
    tiles = own // TILE
    held = q_in.shape[1]
    total = spaces * beads
    spot = space * beads + me
    after = lax.rem(spot + 1, total)
    before = lax.rem(spot + total - 1, total)
    after_id = (lax.div(after, beads), lax.rem(after, beads))
    before_id = (lax.div(before, beads), lax.rem(before, beads))
    peers = [lax.rem(me + d, beads) for d in range(1, beads)]
    order = sorted(range(beads - 1), key=lambda n: -min(n + 1, beads - n - 1))

    barrier = pltpu.get_barrier_semaphore()
    for peer in peers:
        pl.semaphore_signal(barrier, inc=1, device_id=(space, peer), device_id_type=MESH)
    for device in (before_id, after_id):
        pl.semaphore_signal(barrier, inc=1, device_id=device, device_id_type=MESH)

    my_rows = pl.ds(pl.multiple_of(held * me, held), held)
    my_lanes = pl.ds(pl.multiple_of(own * me, own), own)
    local = [
        (q_in, q_stage),
        (p_in, p_stage),
        (q_in.at[:, :, my_lanes], q_all.at[:, my_rows, :]),
        (p_in.at[:, :, my_lanes], p_all.at[:, my_rows, :]),
        (bond_in.at[:, my_lanes], bond_v),
        (angle_in.at[:, pl.ds(pl.multiple_of((own // 2) * me, own // 2), own // 2)], angle_v),
        (mass_in, mass_v),
        (strength_in, strength_v),
        (nbr_in, nbr_s),
        (const_in, const_v),
    ]
    local = [pltpu.make_async_copy(a, b, local_sem.at[n]) for n, (a, b) in enumerate(local)]
    for copy in local:
        copy.start()

    def exchange(kind, source, target):
        copies = []
        for n in order:
            peer = peers[n]
            copies.append(
                pltpu.make_async_remote_copy(
                    src_ref=source(peer),
                    dst_ref=target,
                    send_sem=send_sem.at[kind, n],
                    recv_sem=recv_sem.at[kind, n],
                    device_id=(space, peer),
                    device_id_type=MESH,
                )
            )
        for copy in copies:
            copy.start()
        return copies

    def lanes_of(ref):
        return lambda peer: ref.at[:, :, pl.ds(pl.multiple_of(own * peer, own), own)]

    def rows_of(ref):
        return lambda peer: ref.at[:, pl.ds(pl.multiple_of(held * peer, held), held), :]

    pl.semaphore_wait(barrier, beads + 1)
    local[0].wait()
    sends = exchange(0, lanes_of(q_stage), q_all.at[:, my_rows, :])
    q_sends = list(sends)
    local[1].wait()
    p_sends = exchange(1, lanes_of(p_stage), p_all.at[:, my_rows, :])
    sends = sends + p_sends

    for n in (4, 5, 6, 7, 8, 9):
        local[n].wait()

    place = lax.broadcasted_iota(jnp.int32, (TILE, TILE), 0)
    lane = lax.broadcasted_iota(jnp.int32, (8, TILE), 1)

    def hot(row):
        return jnp.where(place == row, 1.0, 0.0).astype(F32)

    for t in range(tiles):
        ends = bond_v[:, t * TILE : (t + 1) * TILE]
        bonds = hot(ends[0:1]) - hot(ends[1:2])
        pair = angle_v[:, (t // 2) * TILE : (t // 2 + 1) * TILE]
        rows = [jnp.broadcast_to(pair[e : e + 1], (8, TILE)) for e in range(3)]
        turned = [pltpu.roll(r, APT, 1) for r in rows]
        left, right = (rows, turned) if t % 2 == 0 else (turned, rows)
        outer = jnp.where(lane < APT, left[0], right[2])[0:1]
        centre = jnp.where(lane < APT, left[1], right[1])[0:1]
        angles = hot(outer) - hot(centre)
        pick[t] = jnp.concatenate([bonds, angles], axis=1).astype(BF16)
        drop[t] = jnp.concatenate([jnp.transpose(bonds), jnp.transpose(angles)], axis=0).astype(BF16)

    mass_row = jnp.concatenate([mass_v[pl.ds(tiles * me + t, 1), :] for t in range(tiles)], axis=1)
    inverse = 1.0 / mass_row
    strengths = [strength_v[pl.ds(tiles * me + t, 1), :] for t in range(tiles)]

    free_table = const_v[0:64, 0:192]
    narrow_table = const_v[64:80, 0:288]
    wide_table = const_v[80:176, 0:48]

    row16 = lax.broadcasted_iota(jnp.int32, (16, TILE), 0)
    feature = row16 < 12

    def contracted(current):
        high, low = split2(jnp.concatenate(current, axis=0))
        return mm(narrow_table, jnp.concatenate([high, high, low], axis=0))

    def start_halo(turn, narrow):
        for t in range(tiles):
            ext[turn, GT + t] = jnp.where(feature, lanes(narrow, t), strengths[t])
        copies = []
        for side, device, source, target in (
            (0, before_id, GT, GT + tiles),
            (1, after_id, tiles, 0),
        ):
            copies.append(
                pltpu.make_async_remote_copy(
                    src_ref=ext.at[turn, pl.ds(source, GT)],
                    dst_ref=ext.at[turn, pl.ds(target, GT)],
                    send_sem=halo_send.at[turn, side],
                    recv_sem=halo_recv.at[turn, side],
                    device_id=device,
                    device_id_type=MESH,
                )
            )
        for copy in copies:
            copy.start()
        return copies

    scale = math.sqrt(2.0 / range_sq * math.log2(math.e))

    def sides(turn, u, with_own):
        block = ext[turn, u]
        scaled = block * scale
        square = scaled * scaled
        norms = scaled
        for k in range(KEPT):
            part = 0.5 * (square[3 * k : 3 * k + 1] + square[3 * k + 1 : 3 * k + 2] + square[3 * k + 2 : 3 * k + 3])
            norms = jnp.where(row16 == 12 + k, part, norms)
        parts = split3(norms)
        wide_parts = [x.astype(F32) for x in parts]
        ones = [jnp.where(feature, x, 1.0) for x in wide_parts]
        stack = jnp.concatenate(
            [wide_parts[0], wide_parts[1], ones[0], ones[1], wide_parts[2], ones[0], jnp.zeros((32, TILE), F32)], axis=0
        )
        a_side[u] = jnp.transpose(stack).astype(BF16)
        weight = block[12:13]
        g_high, g_low = split2(jnp.where(feature, block * weight, weight))
        g_side[u] = jnp.concatenate([g_high, g_low], axis=0)
        if not with_own:
            return None
        h, m, l = wide_parts

        def own_block(left, right):
            return jnp.where(feature, left, right)

        minus = -jnp.ones_like(h)

        def shift(x):
            return -x

        full = [
            own_block(h, minus),
            own_block(h, minus),
            own_block(m, shift(h)),
            own_block(m, shift(m)),
            own_block(h, minus),
            own_block(l, shift(l)),
        ]
        return full

    def masks():
        found = []
        for k in range(KEPT):
            keep = (row16 >= 3 * k) & (row16 < 3 * k + 3) | (row16 == 12 + k)
            found.append(keep)
        return found

    kept_rows = masks()

    def nonbonded(turn, halo):
        fulls = [sides(turn, GT + t, True) for t in range(tiles)]
        for copy in halo:
            copy.wait_recv()
        for u in list(range(GT)) + list(range(GT + tiles, 2 * GT + tiles)):
            sides(turn, u, False)
        found = []
        base = spot * tiles - GT
        count = total * tiles
        for t in range(tiles):
            rhs = []
            for kp in range(KEPT // 2):
                pair = []
                for k in (2 * kp, 2 * kp + 1):
                    blocks = [jnp.where(kept_rows[k], x, 0.0) for x in fulls[t]]
                    pair.append(jnp.concatenate(blocks + [jnp.zeros((32, TILE), F32)], axis=0))
                rhs.append(jnp.concatenate(pair, axis=1).astype(BF16))
            sums = [None] * (KEPT // 2)
            for j in range(NBR):
                where = jnp.minimum(lax.rem(nbr_s[j, tiles * me + t] - base + count, count), tiles + 2 * GT - 1)
                a = a_side[where]
                g = g_side[where]
                gg = jnp.concatenate([g, g], axis=1)
                for kp in range(KEPT // 2):
                    w = jnp.exp2(mm(a, rhs[kp]))
                    high, low = split2(w)
                    got = mm(gg, jnp.concatenate([high, low], axis=0))
                    sums[kp] = got if sums[kp] is None else sums[kp] + got
            block = ext[turn, GT + t]
            force = jnp.zeros((16, TILE), F32)
            for k in range(KEPT):
                both = sums[k // 2]
                both = both[0:16] + both[16:32]
                both = lanes(both, k % 2)
                force = jnp.where((row16 >= 3 * k) & (row16 < 3 * k + 3), block * both[12:13] - both, force)
            found.append(force * strengths[t])
        high, low = split2(jnp.concatenate(found, axis=1))
        return mm(wide_table, jnp.concatenate([high, high, low], axis=0))

    def bonded(current):
        forces = []
        for t in range(tiles):
            high, low = split2(jnp.concatenate([lanes(x, t) for x in current], axis=0))
            table = pick[t]
            got = mm(jnp.concatenate([high, low], axis=1), jnp.concatenate([table, table], axis=0))
            stretch = [got[c * BEADS : (c + 1) * BEADS, :TILE] for c in range(3)]
            arms = [got[c * BEADS : (c + 1) * BEADS, TILE:] for c in range(3)]
            swapped = [pltpu.roll(x, APT, 1) for x in arms]
            factor = -bond_stiff * (sum(x * x for x in stretch) - bond_rest)
            bend = -angle_stiff * (sum(x * y for x, y in zip(arms, swapped)) - angle_rest)
            push = jnp.concatenate(
                [jnp.concatenate([factor * x, bend * y], axis=1) for x, y in zip(stretch, swapped)], axis=0
            )
            high, low = split2(push)
            back = drop[t]
            forces.append(mm(jnp.concatenate([high, low], axis=1), jnp.concatenate([back, back], axis=0)))
        return [
            jnp.concatenate([f[c * BEADS : (c + 1) * BEADS] for f in forces], axis=1) for c in range(3)
        ]

    def advance(current, speed):
        moved, fast = [], []
        for c in range(3):
            first = current[c][0:1]
            both = jnp.concatenate([current[c] - first, speed[c]], axis=0)
            high, low = split2(both)
            got = mm(free_table, jnp.concatenate([high, high, low], axis=0))
            moved.append(first + got[:BEADS])
            fast.append(got[BEADS:])
        return moved, fast

    half = 0.5 * time_step / SUBS

    local[2].wait()
    for copy in q_sends:
        copy.wait_recv()
    current = [q_all[c] for c in range(3)]
    halo = start_halo(0, contracted(current))
    pushed = bonded(current)
    kick = nonbonded(0, halo)
    halos = list(halo)
    kicks = [kick[c * BEADS : (c + 1) * BEADS] for c in range(3)]

    local[3].wait()
    for copy in p_sends:
        copy.wait_recv()
    speed = [(p_all[c] + half * pushed[c] + kicks[c]) * inverse for c in range(3)]
    for substep in range(SUBS):
        current, speed = advance(current, speed)
        if substep + 1 < SUBS:
            pushed = bonded(current)
            speed = [speed[c] + (2.0 * half) * pushed[c] * inverse for c in range(3)]

    halo = start_halo(1, contracted(current))
    halos = halos + list(halo)
    for c in range(3):
        q_done[c] = current[c]
    sends = sends + exchange(2, rows_of(q_done), q_out.at[:, :, my_lanes])
    mine_q = pltpu.make_async_copy(q_done.at[:, my_rows, :], q_out.at[:, :, my_lanes], own_sem.at[0])
    mine_q.start()
    pushed = bonded(current)
    moment = [speed[c] * mass_row + half * pushed[c] for c in range(3)]
    kick = nonbonded(1, halo)
    for c in range(3):
        p_done[c] = moment[c] + kick[c * BEADS : (c + 1) * BEADS]
    late = exchange(3, rows_of(p_done), p_out.at[:, :, my_lanes])
    mine_p = pltpu.make_async_copy(p_done.at[:, my_rows, :], p_out.at[:, :, my_lanes], own_sem.at[1])
    mine_p.start()
    for copy in sends:
        copy.wait_send()
    for copy in halos:
        copy.wait_send()
    for copy in sends[2 * (beads - 1) :]:
        copy.wait_recv()
    mine_q.wait()
    mine_p.wait()
    for copy in late:
        copy.wait()


def solution(mesh):
    spaces, beads = mesh.shape["space"], mesh.shape["bead"]
    table = constant_table()

    def body(positions, momenta, masses, strengths, bond_ends, angle_ends, neighbour_tiles):
        held, _, slab = positions.shape
        own = slab // beads
        tiles = own // TILE
        near = tiles + 2 * GT
        moved = jax.ShapeDtypeStruct((3, held, slab), F32)
        anywhere = pl.BlockSpec(memory_space=pl.ANY)
        done = pl.pallas_call(
            functools.partial(kernel, spaces, beads),
            out_shape=(moved, moved),
            in_specs=[anywhere] * 8,
            out_specs=(anywhere, anywhere),
            scratch_shapes=[
                pltpu.VMEM((3, held, slab), F32),
                pltpu.VMEM((3, held, slab), F32),
                pltpu.VMEM((3, BEADS, own), F32),
                pltpu.VMEM((3, BEADS, own), F32),
                pltpu.VMEM((3, BEADS, own), F32),
                pltpu.VMEM((3, BEADS, own), F32),
                pltpu.VMEM((slab // TILE, TILE), F32),
                pltpu.VMEM((slab // TILE, TILE), F32),
                pltpu.VMEM((2, own), jnp.int32),
                pltpu.VMEM((3, own // 2), jnp.int32),
                pltpu.SMEM((NBR, slab // TILE), jnp.int32),
                pltpu.VMEM(table.shape, BF16),
                pltpu.VMEM((tiles, TILE, 2 * TILE), BF16),
                pltpu.VMEM((tiles, 2 * TILE, TILE), BF16),
                pltpu.VMEM((2, near, 16, TILE), F32),
                pltpu.VMEM((near, TILE, TILE), BF16),
                pltpu.VMEM((near, 32, TILE), BF16),
                pltpu.SemaphoreType.DMA((10,)),
                pltpu.SemaphoreType.DMA((4, beads - 1)),
                pltpu.SemaphoreType.DMA((4, beads - 1)),
                pltpu.SemaphoreType.DMA((2,)),
                pltpu.SemaphoreType.DMA((2, 2)),
                pltpu.SemaphoreType.DMA((2, 2)),
            ],
            compiler_params=pltpu.CompilerParams(collective_id=0, has_side_effects=True),
        )(
            jnp.transpose(positions, (1, 0, 2)),
            jnp.transpose(momenta, (1, 0, 2)),
            masses.reshape(-1, TILE),
            strengths.reshape(-1, TILE),
            bond_ends,
            angle_ends,
            neighbour_tiles,
            jnp.asarray(table),
        )
        return tuple(jnp.transpose(x, (1, 0, 2)) for x in done)

    placed = (
        P("bead", None, "space"),
        P("bead", None, "space"),
        P("space"),
        P("space"),
        P(None, "space"),
        P(None, "space"),
        P(None, "space"),
    )
    return jax.shard_map(
        body,
        mesh=mesh,
        in_specs=placed,
        out_specs=(P("bead", None, "space"), P("bead", None, "space")),
        check_vma=False,
    )
```

```python
import functools
import math

import jax
import jax.numpy as jnp
import ml_dtypes
import numpy as np
from jax import lax
from jax.experimental import pallas as pl
from jax.experimental.pallas import tpu as pltpu
from jax.sharding import PartitionSpec as P

BEADS = 32
KEPT = 4
SUBS = 3
TILE = 128
GT = 2
NBR = 3
BPT = 128
APT = 64

time_step = 0.3
spring_freq = 80.0
bond_stiff = 0.2
bond_rest = 1.0
angle_stiff = 0.1
angle_rest = 0.5
range_sq = 4.0

F32 = jnp.float32
BF16 = jnp.bfloat16
MESH = pl.DeviceIdType.MESH


def mode_table(number):
    within = np.arange(number)
    result = np.zeros((number, number))
    for column in range(number):
        if column == 0:
            result[:, column] = 1.0 / math.sqrt(number)
        elif 2 * column < number:
            result[:, column] = math.sqrt(2.0 / number) * np.cos(2 * np.pi * within * column / number)
        elif 2 * column == number:
            result[:, column] = (-1.0) ** within / math.sqrt(number)
        else:
            result[:, column] = math.sqrt(2.0 / number) * np.sin(2 * np.pi * within * column / number)
    return result


def contract_table(number, kept):
    larger = mode_table(number)
    smaller = mode_table(kept)
    chosen = [column if 2 * column <= kept else number - kept + column for column in range(kept)]
    return math.sqrt(kept / number) * smaller @ larger[:, chosen].T


def halves(table):
    high = table.astype(ml_dtypes.bfloat16)
    low = (table - high.astype(np.float64)).astype(ml_dtypes.bfloat16)
    return high, low


def three_products(table):
    high, low = halves(table)
    return np.concatenate([high, low, high], axis=1)


def constant_table():
    modes = mode_table(BEADS)
    interval = time_step / SUBS
    freqs = 2.0 * spring_freq * np.sin(np.pi * np.arange(BEADS) / BEADS)
    safe = np.where(freqs > 0, freqs, 1.0)
    cosine = np.cos(freqs * interval)
    gains = np.where(freqs > 0, np.sin(freqs * interval) / safe, interval)
    drags = freqs * np.sin(freqs * interval)
    keep = (modes * cosine) @ modes.T
    gain = (modes * gains) @ modes.T
    drag = -(modes * drags) @ modes.T
    free = np.block([[keep, gain], [drag, keep]])
    contract = contract_table(BEADS, KEPT)
    narrow = np.zeros((16, 3 * BEADS))
    for k in range(KEPT):
        for c in range(3):
            narrow[3 * k + c, c * BEADS : (c + 1) * BEADS] = contract[k]
    expand = BEADS / KEPT * contract.T
    wide = np.zeros((3 * BEADS, 16))
    for k in range(KEPT):
        for c in range(3):
            wide[c * BEADS : (c + 1) * BEADS, 3 * k + c] = expand[:, k]
    wide *= 0.5 * time_step * 2.0 / range_sq
    table = np.zeros((64 + 16 + 96, 384), ml_dtypes.bfloat16)
    table[:64, :192] = three_products(free)
    table[64:80, :288] = three_products(narrow)
    table[80:176, :48] = three_products(wide)
    return table


def split2(x):
    high = x.astype(BF16)
    return high, (x - high.astype(F32)).astype(BF16)


def split3(x):
    high = x.astype(BF16)
    rest = x - high.astype(F32)
    middle = rest.astype(BF16)
    return high, middle, (rest - middle.astype(F32)).astype(BF16)


def mm(a, b):
    return jnp.dot(a, b, preferred_element_type=F32)


def lanes(x, t):
    return x[:, t * TILE : (t + 1) * TILE]


def walk(space, place, beads):
    core = lax.rem(space, 2)
    return core * (beads - 1) + (1 - 2 * core) * place


def flip(space):
    return 1 - lax.rem(lax.div(space, 2), 2)


def block_of(space, bead, beads):
    row = lax.div(bead, 2)
    return walk(space, 2 * row + lax.rem(bead + row + flip(space), 2), beads)


def device_of(spot, beads):
    space = lax.div(spot, beads)
    place = walk(space, lax.rem(spot, beads), beads)
    row = lax.div(place, 2)
    return space, 2 * row + lax.rem(place + row + flip(space), 2)


def kernel(
    spaces,
    beads,
    q_in,
    p_in,
    mass_in,
    strength_in,
    bond_in,
    angle_in,
    nbr_in,
    const_in,
    q_out,
    p_out,
    q_stage,
    p_stage,
    q_all,
    p_all,
    q_done,
    p_done,
    mass_v,
    strength_v,
    bond_v,
    angle_v,
    nbr_s,
    const_v,
    pick,
    drop,
    ext,
    a_side,
    g_side,
    local_sem,
    send_sem,
    recv_sem,
    own_sem,
    halo_send,
    halo_recv,
):
    space = lax.axis_index("space")
    me = lax.axis_index("bead")
    slab = q_in.shape[2]
    own = slab // beads
    tiles = own // TILE
    held = q_in.shape[1]
    total = spaces * beads
    block = block_of(space, me, beads)
    spot = space * beads + block
    after_id = device_of(lax.rem(spot + 1, total), beads)
    before_id = device_of(lax.rem(spot + total - 1, total), beads)
    peers = [lax.rem(me + d, beads) for d in range(1, beads)]
    order = sorted(range(beads - 1), key=lambda n: -min(n + 1, beads - n - 1))

    barrier = pltpu.get_barrier_semaphore()
    for peer in peers:
        pl.semaphore_signal(barrier, inc=1, device_id=(space, peer), device_id_type=MESH)
    for device in (before_id, after_id):
        pl.semaphore_signal(barrier, inc=1, device_id=device, device_id_type=MESH)

    my_rows = pl.ds(pl.multiple_of(held * me, held), held)
    my_lanes = pl.ds(pl.multiple_of(own * block, own), own)
    local = [
        (q_in, q_stage),
        (p_in, p_stage),
        (q_in.at[:, :, my_lanes], q_all.at[:, my_rows, :]),
        (p_in.at[:, :, my_lanes], p_all.at[:, my_rows, :]),
        (bond_in.at[:, my_lanes], bond_v),
        (angle_in.at[:, pl.ds(pl.multiple_of((own // 2) * block, own // 2), own // 2)], angle_v),
        (mass_in, mass_v),
        (strength_in, strength_v),
        (nbr_in, nbr_s),
        (const_in, const_v),
    ]
    local = [pltpu.make_async_copy(a, b, local_sem.at[n]) for n, (a, b) in enumerate(local)]
    for copy in local:
        copy.start()

    def exchange(kind, source, target):
        copies = []
        for n in order:
            peer = peers[n]
            copies.append(
                pltpu.make_async_remote_copy(
                    src_ref=source(peer),
                    dst_ref=target,
                    send_sem=send_sem.at[kind, n],
                    recv_sem=recv_sem.at[kind, n],
                    device_id=(space, peer),
                    device_id_type=MESH,
                )
            )
        for copy in copies:
            copy.start()
        return copies

    def lanes_of(ref):
        return lambda peer: ref.at[:, :, pl.ds(pl.multiple_of(own * block_of(space, peer, beads), own), own)]

    def rows_of(ref):
        return lambda peer: ref.at[:, pl.ds(pl.multiple_of(held * peer, held), held), :]

    pl.semaphore_wait(barrier, beads + 1)
    local[0].wait()
    sends = exchange(0, lanes_of(q_stage), q_all.at[:, my_rows, :])
    q_sends = list(sends)
    local[1].wait()
    p_sends = exchange(1, lanes_of(p_stage), p_all.at[:, my_rows, :])
    sends = sends + p_sends

    for n in (4, 5, 6, 7, 8, 9):
        local[n].wait()

    place = lax.broadcasted_iota(jnp.int32, (TILE, TILE), 0)
    lane = lax.broadcasted_iota(jnp.int32, (8, TILE), 1)

    def hot(row):
        return jnp.where(place == row, 1.0, 0.0).astype(F32)

    for t in range(tiles):
        ends = bond_v[:, t * TILE : (t + 1) * TILE]
        bonds = hot(ends[0:1]) - hot(ends[1:2])
        pair = angle_v[:, (t // 2) * TILE : (t // 2 + 1) * TILE]
        rows = [jnp.broadcast_to(pair[e : e + 1], (8, TILE)) for e in range(3)]
        turned = [pltpu.roll(r, APT, 1) for r in rows]
        left, right = (rows, turned) if t % 2 == 0 else (turned, rows)
        outer = jnp.where(lane < APT, left[0], right[2])[0:1]
        centre = jnp.where(lane < APT, left[1], right[1])[0:1]
        angles = hot(outer) - hot(centre)
        pick[t] = jnp.concatenate([bonds, angles], axis=1).astype(BF16)
        drop[t] = jnp.concatenate([jnp.transpose(bonds), jnp.transpose(angles)], axis=0).astype(BF16)

    mass_row = jnp.concatenate([mass_v[pl.ds(tiles * block + t, 1), :] for t in range(tiles)], axis=1)
    inverse = 1.0 / mass_row
    strengths = [strength_v[pl.ds(tiles * block + t, 1), :] for t in range(tiles)]

    free_table = const_v[0:64, 0:192]
    narrow_table = const_v[64:80, 0:288]
    wide_table = const_v[80:176, 0:48]

    row16 = lax.broadcasted_iota(jnp.int32, (16, TILE), 0)
    feature = row16 < 12

    def contracted(current):
        high, low = split2(jnp.concatenate(current, axis=0))
        return mm(narrow_table, jnp.concatenate([high, high, low], axis=0))

    def start_halo(turn, narrow):
        for t in range(tiles):
            ext[turn, GT + t] = jnp.where(feature, lanes(narrow, t), strengths[t])
        copies = []
        for side, device, source, target in (
            (0, before_id, GT, GT + tiles),
            (1, after_id, tiles, 0),
        ):
            copies.append(
                pltpu.make_async_remote_copy(
                    src_ref=ext.at[turn, pl.ds(source, GT)],
                    dst_ref=ext.at[turn, pl.ds(target, GT)],
                    send_sem=halo_send.at[turn, side],
                    recv_sem=halo_recv.at[turn, side],
                    device_id=device,
                    device_id_type=MESH,
                )
            )
        for copy in copies:
            copy.start()
        return copies

    scale = math.sqrt(2.0 / range_sq * math.log2(math.e))

    def sides(turn, u, with_own):
        rows = ext[turn, u]
        scaled = rows * scale
        square = scaled * scaled
        norms = scaled
        for k in range(KEPT):
            part = 0.5 * (square[3 * k : 3 * k + 1] + square[3 * k + 1 : 3 * k + 2] + square[3 * k + 2 : 3 * k + 3])
            norms = jnp.where(row16 == 12 + k, part, norms)
        parts = split3(norms)
        wide_parts = [x.astype(F32) for x in parts]
        ones = [jnp.where(feature, x, 1.0) for x in wide_parts]
        stack = jnp.concatenate(
            [wide_parts[0], wide_parts[1], ones[0], ones[1], wide_parts[2], ones[0], jnp.zeros((32, TILE), F32)], axis=0
        )
        a_side[u] = jnp.transpose(stack).astype(BF16)
        weight = rows[12:13]
        g_high, g_low = split2(jnp.where(feature, rows * weight, weight))
        g_side[u] = jnp.concatenate([g_high, g_low], axis=0)
        if not with_own:
            return None
        h, m, l = wide_parts

        def own_block(left, right):
            return jnp.where(feature, left, right)

        minus = -jnp.ones_like(h)

        def shift(x):
            return -x

        full = [
            own_block(h, minus),
            own_block(h, minus),
            own_block(m, shift(h)),
            own_block(m, shift(m)),
            own_block(h, minus),
            own_block(l, shift(l)),
        ]
        return full

    def masks():
        found = []
        for k in range(KEPT):
            keep = (row16 >= 3 * k) & (row16 < 3 * k + 3) | (row16 == 12 + k)
            found.append(keep)
        return found

    kept_rows = masks()

    def nonbonded(turn, halo):
        fulls = [sides(turn, GT + t, True) for t in range(tiles)]
        for copy in halo:
            copy.wait_recv()
        for u in list(range(GT)) + list(range(GT + tiles, 2 * GT + tiles)):
            sides(turn, u, False)
        found = []
        base = spot * tiles - GT
        count = total * tiles
        for t in range(tiles):
            rhs = []
            for kp in range(KEPT // 2):
                pair = []
                for k in (2 * kp, 2 * kp + 1):
                    blocks = [jnp.where(kept_rows[k], x, 0.0) for x in fulls[t]]
                    pair.append(jnp.concatenate(blocks + [jnp.zeros((32, TILE), F32)], axis=0))
                rhs.append(jnp.concatenate(pair, axis=1).astype(BF16))
            sums = [None] * (KEPT // 2)
            for j in range(NBR):
                where = jnp.minimum(lax.rem(nbr_s[j, tiles * block + t] - base + count, count), tiles + 2 * GT - 1)
                a = a_side[where]
                g = g_side[where]
                gg = jnp.concatenate([g, g], axis=1)
                for kp in range(KEPT // 2):
                    w = jnp.exp2(mm(a, rhs[kp]))
                    high, low = split2(w)
                    got = mm(gg, jnp.concatenate([high, low], axis=0))
                    sums[kp] = got if sums[kp] is None else sums[kp] + got
            rows = ext[turn, GT + t]
            force = jnp.zeros((16, TILE), F32)
            for k in range(KEPT):
                both = sums[k // 2]
                both = both[0:16] + both[16:32]
                both = lanes(both, k % 2)
                force = jnp.where((row16 >= 3 * k) & (row16 < 3 * k + 3), rows * both[12:13] - both, force)
            found.append(force * strengths[t])
        high, low = split2(jnp.concatenate(found, axis=1))
        return mm(wide_table, jnp.concatenate([high, high, low], axis=0))

    def bonded(current):
        forces = []
        for t in range(tiles):
            high, low = split2(jnp.concatenate([lanes(x, t) for x in current], axis=0))
            table = pick[t]
            got = mm(jnp.concatenate([high, low], axis=1), jnp.concatenate([table, table], axis=0))
            stretch = [got[c * BEADS : (c + 1) * BEADS, :TILE] for c in range(3)]
            arms = [got[c * BEADS : (c + 1) * BEADS, TILE:] for c in range(3)]
            swapped = [pltpu.roll(x, APT, 1) for x in arms]
            factor = -bond_stiff * (sum(x * x for x in stretch) - bond_rest)
            bend = -angle_stiff * (sum(x * y for x, y in zip(arms, swapped)) - angle_rest)
            push = jnp.concatenate(
                [jnp.concatenate([factor * x, bend * y], axis=1) for x, y in zip(stretch, swapped)], axis=0
            )
            high, low = split2(push)
            back = drop[t]
            forces.append(mm(jnp.concatenate([high, low], axis=1), jnp.concatenate([back, back], axis=0)))
        return [
            jnp.concatenate([f[c * BEADS : (c + 1) * BEADS] for f in forces], axis=1) for c in range(3)
        ]

    def advance(current, speed):
        moved, fast = [], []
        for c in range(3):
            first = current[c][0:1]
            both = jnp.concatenate([current[c] - first, speed[c]], axis=0)
            high, low = split2(both)
            got = mm(free_table, jnp.concatenate([high, high, low], axis=0))
            moved.append(first + got[:BEADS])
            fast.append(got[BEADS:])
        return moved, fast

    half = 0.5 * time_step / SUBS

    local[2].wait()
    for copy in q_sends:
        copy.wait_recv()
    current = [q_all[c] for c in range(3)]
    halo = start_halo(0, contracted(current))
    pushed = bonded(current)
    kick = nonbonded(0, halo)
    halos = list(halo)
    kicks = [kick[c * BEADS : (c + 1) * BEADS] for c in range(3)]

    local[3].wait()
    for copy in p_sends:
        copy.wait_recv()
    speed = [(p_all[c] + half * pushed[c] + kicks[c]) * inverse for c in range(3)]
    for substep in range(SUBS):
        current, speed = advance(current, speed)
        if substep + 1 < SUBS:
            pushed = bonded(current)
            speed = [speed[c] + (2.0 * half) * pushed[c] * inverse for c in range(3)]

    halo = start_halo(1, contracted(current))
    halos = halos + list(halo)
    for c in range(3):
        q_done[c] = current[c]
    sends = sends + exchange(2, rows_of(q_done), q_out.at[:, :, my_lanes])
    mine_q = pltpu.make_async_copy(q_done.at[:, my_rows, :], q_out.at[:, :, my_lanes], own_sem.at[0])
    mine_q.start()
    pushed = bonded(current)
    moment = [speed[c] * mass_row + half * pushed[c] for c in range(3)]
    kick = nonbonded(1, halo)
    for c in range(3):
        p_done[c] = moment[c] + kick[c * BEADS : (c + 1) * BEADS]
    late = exchange(3, rows_of(p_done), p_out.at[:, :, my_lanes])
    mine_p = pltpu.make_async_copy(p_done.at[:, my_rows, :], p_out.at[:, :, my_lanes], own_sem.at[1])
    mine_p.start()
    for copy in sends:
        copy.wait_send()
    for copy in halos:
        copy.wait_send()
    for copy in sends[2 * (beads - 1) :]:
        copy.wait_recv()
    mine_q.wait()
    mine_p.wait()
    for copy in late:
        copy.wait()


def solution(mesh):
    spaces, beads = mesh.shape["space"], mesh.shape["bead"]
    table = constant_table()

    def body(positions, momenta, masses, strengths, bond_ends, angle_ends, neighbour_tiles):
        held, _, slab = positions.shape
        own = slab // beads
        tiles = own // TILE
        near = tiles + 2 * GT
        moved = pltpu.VMEM((3, held, slab), F32)
        anywhere = pl.BlockSpec(memory_space=pl.ANY)
        done = pl.pallas_call(
            functools.partial(kernel, spaces, beads),
            out_shape=(moved, moved),
            in_specs=[anywhere] * 8,
            out_specs=(pl.BlockSpec(memory_space=pltpu.VMEM),) * 2,
            scratch_shapes=[
                pltpu.VMEM((3, held, slab), F32),
                pltpu.VMEM((3, held, slab), F32),
                pltpu.VMEM((3, BEADS, own), F32),
                pltpu.VMEM((3, BEADS, own), F32),
                pltpu.VMEM((3, BEADS, own), F32),
                pltpu.VMEM((3, BEADS, own), F32),
                pltpu.VMEM((slab // TILE, TILE), F32),
                pltpu.VMEM((slab // TILE, TILE), F32),
                pltpu.VMEM((2, own), jnp.int32),
                pltpu.VMEM((3, own // 2), jnp.int32),
                pltpu.SMEM((NBR, slab // TILE), jnp.int32),
                pltpu.VMEM(table.shape, BF16),
                pltpu.VMEM((tiles, TILE, 2 * TILE), BF16),
                pltpu.VMEM((tiles, 2 * TILE, TILE), BF16),
                pltpu.VMEM((2, near, 16, TILE), F32),
                pltpu.VMEM((near, TILE, TILE), BF16),
                pltpu.VMEM((near, 32, TILE), BF16),
                pltpu.SemaphoreType.DMA((10,)),
                pltpu.SemaphoreType.DMA((4, beads - 1)),
                pltpu.SemaphoreType.DMA((4, beads - 1)),
                pltpu.SemaphoreType.DMA((2,)),
                pltpu.SemaphoreType.DMA((2, 2)),
                pltpu.SemaphoreType.DMA((2, 2)),
            ],
            compiler_params=pltpu.CompilerParams(collective_id=0, has_side_effects=True),
        )(
            jnp.transpose(positions, (1, 0, 2)),
            jnp.transpose(momenta, (1, 0, 2)),
            masses.reshape(-1, TILE),
            strengths.reshape(-1, TILE),
            bond_ends,
            angle_ends,
            neighbour_tiles,
            jnp.asarray(table),
        )
        return tuple(jnp.transpose(x, (1, 0, 2)) for x in done)

    placed = (
        P("bead", None, "space"),
        P("bead", None, "space"),
        P("space"),
        P("space"),
        P(None, "space"),
        P(None, "space"),
        P(None, "space"),
    )
    return jax.shard_map(
        body,
        mesh=mesh,
        in_specs=placed,
        out_specs=(P("bead", None, "space"), P("bead", None, "space")),
        check_vma=False,
    )
```

```python
import functools
import math

import jax
import jax.numpy as jnp
import ml_dtypes
import numpy as np
from jax import lax
from jax.experimental import pallas as pl
from jax.experimental.pallas import tpu as pltpu
from jax.sharding import PartitionSpec as P

BEADS = 32
KEPT = 4
SUBS = 3
TILE = 128
GT = 2
NBR = 3
BPT = 128
APT = 64

time_step = 0.3
spring_freq = 80.0
bond_stiff = 0.2
bond_rest = 1.0
angle_stiff = 0.1
angle_rest = 0.5
range_sq = 4.0
CHUNK = 2
GROUP = 4

F32 = jnp.float32
BF16 = jnp.bfloat16
MESH = pl.DeviceIdType.MESH


def mode_table(number):
    within = np.arange(number)
    result = np.zeros((number, number))
    for column in range(number):
        if column == 0:
            result[:, column] = 1.0 / math.sqrt(number)
        elif 2 * column < number:
            result[:, column] = math.sqrt(2.0 / number) * np.cos(2 * np.pi * within * column / number)
        elif 2 * column == number:
            result[:, column] = (-1.0) ** within / math.sqrt(number)
        else:
            result[:, column] = math.sqrt(2.0 / number) * np.sin(2 * np.pi * within * column / number)
    return result


def contract_table(number, kept):
    larger = mode_table(number)
    smaller = mode_table(kept)
    chosen = [column if 2 * column <= kept else number - kept + column for column in range(kept)]
    return math.sqrt(kept / number) * smaller @ larger[:, chosen].T


def halves(table):
    high = table.astype(ml_dtypes.bfloat16)
    low = (table - high.astype(np.float64)).astype(ml_dtypes.bfloat16)
    return high, low


def three_products(table):
    high, low = halves(table)
    return np.concatenate([high, low, high], axis=1)


def constant_table():
    modes = mode_table(BEADS)
    interval = time_step / SUBS
    freqs = 2.0 * spring_freq * np.sin(np.pi * np.arange(BEADS) / BEADS)
    safe = np.where(freqs > 0, freqs, 1.0)
    cosine = np.cos(freqs * interval)
    gains = np.where(freqs > 0, np.sin(freqs * interval) / safe, interval)
    drags = freqs * np.sin(freqs * interval)
    keep = (modes * cosine) @ modes.T
    gain = (modes * gains) @ modes.T
    drag = -(modes * drags) @ modes.T
    free = np.block([[keep, gain], [drag, keep]])
    contract = contract_table(BEADS, KEPT)
    narrow = np.zeros((16, 3 * BEADS))
    for k in range(KEPT):
        for c in range(3):
            narrow[3 * k + c, c * BEADS : (c + 1) * BEADS] = contract[k]
    expand = BEADS / KEPT * contract.T
    wide = np.zeros((3 * BEADS, 16))
    for k in range(KEPT):
        for c in range(3):
            wide[c * BEADS : (c + 1) * BEADS, 3 * k + c] = expand[:, k]
    wide *= 0.5 * time_step * 2.0 / range_sq
    table = np.zeros((64 + 16 + 96, 384), ml_dtypes.bfloat16)
    table[:64, :192] = three_products(free)
    table[64:80, :288] = three_products(narrow)
    table[80:176, :48] = three_products(wide)
    return table


def split2(x):
    high = x.astype(BF16)
    return high, (x - high.astype(F32)).astype(BF16)


def split3(x):
    high = x.astype(BF16)
    rest = x - high.astype(F32)
    middle = rest.astype(BF16)
    return high, middle, (rest - middle.astype(F32)).astype(BF16)


def mm(a, b):
    return jnp.dot(a, b, preferred_element_type=F32)


def lanes(x, t):
    return x[:, t * TILE : (t + 1) * TILE]


def walk(space, place, beads):
    core = lax.rem(space, 2)
    return core * (beads - 1) + (1 - 2 * core) * place


def flip(space):
    return 1 - lax.rem(lax.div(space, 2), 2)


def block_of(space, bead, beads):
    row = lax.div(bead, 2)
    return walk(space, 2 * row + lax.rem(bead + row + flip(space), 2), beads)


def device_of(spot, beads):
    space = lax.div(spot, beads)
    place = walk(space, lax.rem(spot, beads), beads)
    row = lax.div(place, 2)
    return space, 2 * row + lax.rem(place + row + flip(space), 2)


def kernel(
    spaces,
    beads,
    q_in,
    p_in,
    mass_in,
    strength_in,
    bond_in,
    angle_in,
    nbr_in,
    const_in,
    q_out,
    p_out,
    q_stage,
    p_stage,
    q_all,
    p_all,
    q_done,
    p_done,
    mass_v,
    strength_v,
    bond_v,
    angle_v,
    nbr_s,
    const_v,
    pick,
    drop,
    ext,
    a_side,
    g_side,
    local_sem,
    send_sem,
    recv_sem,
    own_sem,
    halo_send,
    halo_recv,
):
    space = lax.axis_index("space")
    me = lax.axis_index("bead")
    slab = q_in.shape[2]
    own = slab // beads
    tiles = own // TILE
    held = q_in.shape[1]
    total = spaces * beads
    block = block_of(space, me, beads)
    spot = space * beads + block
    after_id = device_of(lax.rem(spot + 1, total), beads)
    before_id = device_of(lax.rem(spot + total - 1, total), beads)
    peers = [lax.rem(me + d, beads) for d in range(1, beads)]
    order = sorted(range(beads - 1), key=lambda n: -min(n + 1, beads - n - 1))

    early = pltpu.make_async_copy(q_in, q_stage, local_sem.at[0])
    early.start()
    barrier = pltpu.get_barrier_semaphore()
    for peer in peers:
        pl.semaphore_signal(barrier, inc=1, device_id=(space, peer), device_id_type=MESH)
    for device in (before_id, after_id):
        pl.semaphore_signal(barrier, inc=1, device_id=device, device_id_type=MESH)

    my_rows = pl.ds(pl.multiple_of(held * me, held), held)
    my_lanes = pl.ds(pl.multiple_of(own * block, own), own)
    local = [
        (q_in, q_stage),
        (p_in, p_stage),
        (q_in.at[:, :, my_lanes], q_all.at[:, my_rows, :]),
        (p_in.at[:, :, my_lanes], p_all.at[:, my_rows, :]),
        (bond_in.at[:, my_lanes], bond_v),
        (angle_in.at[:, pl.ds(pl.multiple_of((own // 2) * block, own // 2), own // 2)], angle_v),
        (mass_in, mass_v),
        (strength_in, strength_v),
        (nbr_in, nbr_s),
        (const_in, const_v),
    ]
    local = [pltpu.make_async_copy(a, b, local_sem.at[n]) for n, (a, b) in enumerate(local)]
    for copy in local[1:]:
        copy.start()

    def exchange(kind, source, target):
        copies = []
        for n in order:
            peer = peers[n]
            copies.append(
                pltpu.make_async_remote_copy(
                    src_ref=source(peer),
                    dst_ref=target,
                    send_sem=send_sem.at[kind, n],
                    recv_sem=recv_sem.at[kind, n],
                    device_id=(space, peer),
                    device_id_type=MESH,
                )
            )
        for copy in copies:
            copy.start()
        return copies

    def lanes_of(ref):
        return lambda peer: ref.at[:, :, pl.ds(pl.multiple_of(own * block_of(space, peer, beads), own), own)]

    def rows_of(ref):
        return lambda peer: ref.at[:, pl.ds(pl.multiple_of(held * peer, held), held), :]

    pl.semaphore_wait(barrier, beads + 1)
    local[0].wait()
    sends = exchange(0, lanes_of(q_stage), q_all.at[:, my_rows, :])
    q_sends = list(sends)
    local[1].wait()
    p_sends = exchange(1, lanes_of(p_stage), p_all.at[:, my_rows, :])
    sends = sends + p_sends

    for n in (4, 5, 6, 7, 8, 9):
        local[n].wait()

    place = lax.broadcasted_iota(jnp.int32, (TILE, TILE), 0)
    lane = lax.broadcasted_iota(jnp.int32, (8, TILE), 1)

    def hot(row):
        return jnp.where(place == row, 1.0, 0.0).astype(F32)

    for t in range(tiles):
        ends = bond_v[:, t * TILE : (t + 1) * TILE]
        bonds = hot(ends[0:1]) - hot(ends[1:2])
        pair = angle_v[:, (t // 2) * TILE : (t // 2 + 1) * TILE]
        rows = [jnp.broadcast_to(pair[e : e + 1], (8, TILE)) for e in range(3)]
        turned = [pltpu.roll(r, APT, 1) for r in rows]
        left, right = (rows, turned) if t % 2 == 0 else (turned, rows)
        outer = jnp.where(lane < APT, left[0], right[2])[0:1]
        centre = jnp.where(lane < APT, left[1], right[1])[0:1]
        angles = hot(outer) - hot(centre)
        pick[t] = jnp.concatenate([bonds, angles], axis=1).astype(BF16)
        drop[t] = jnp.concatenate([jnp.transpose(bonds), jnp.transpose(angles)], axis=0).astype(BF16)

    mass_row = jnp.concatenate([mass_v[pl.ds(tiles * block + t, 1), :] for t in range(tiles)], axis=1)
    inverse = 1.0 / mass_row
    strengths = [strength_v[pl.ds(tiles * block + t, 1), :] for t in range(tiles)]

    free_table = const_v[0:64, 0:192]
    narrow_table = const_v[64:80, 0:288]
    wide_table = const_v[80:176, 0:48]

    row16 = lax.broadcasted_iota(jnp.int32, (16, TILE), 0)
    feature = row16 < 12

    def contracted(current):
        high, low = split2(jnp.concatenate(current, axis=0))
        return mm(narrow_table, jnp.concatenate([high, high, low], axis=0))

    def start_halo(turn, narrow):
        for t in range(tiles):
            ext[turn, GT + t] = jnp.where(feature, lanes(narrow, t), strengths[t])
        copies = []
        for side, device, source, target in (
            (0, before_id, GT, GT + tiles),
            (1, after_id, tiles, 0),
        ):
            copies.append(
                pltpu.make_async_remote_copy(
                    src_ref=ext.at[turn, pl.ds(source, GT)],
                    dst_ref=ext.at[turn, pl.ds(target, GT)],
                    send_sem=halo_send.at[turn, side],
                    recv_sem=halo_recv.at[turn, side],
                    device_id=device,
                    device_id_type=MESH,
                )
            )
        for copy in copies:
            copy.start()
        return copies

    scale = math.sqrt(2.0 / range_sq * math.log2(math.e))

    def sides(turn, u, with_own):
        rows = ext[turn, u]
        scaled = rows * scale
        square = scaled * scaled
        norms = scaled
        for k in range(KEPT):
            part = 0.5 * (square[3 * k : 3 * k + 1] + square[3 * k + 1 : 3 * k + 2] + square[3 * k + 2 : 3 * k + 3])
            norms = jnp.where(row16 == 12 + k, part, norms)
        parts = split3(norms)
        wide_parts = [x.astype(F32) for x in parts]
        ones = [jnp.where(feature, x, 1.0) for x in wide_parts]
        stack = jnp.concatenate(
            [wide_parts[0], wide_parts[1], ones[0], ones[1], wide_parts[2], ones[0], jnp.zeros((32, TILE), F32)], axis=0
        )
        a_side[u] = jnp.transpose(stack).astype(BF16)
        weight = rows[12:13]
        g_high, g_low = split2(jnp.where(feature, rows * weight, weight))
        g_side[u] = jnp.concatenate([g_high, g_low], axis=0)
        if not with_own:
            return None
        h, m, l = wide_parts

        def own_block(left, right):
            return jnp.where(feature, left, right)

        minus = -jnp.ones_like(h)

        def shift(x):
            return -x

        full = [
            own_block(h, minus),
            own_block(h, minus),
            own_block(m, shift(h)),
            own_block(m, shift(m)),
            own_block(h, minus),
            own_block(l, shift(l)),
        ]
        return full

    def masks():
        found = []
        for k in range(KEPT):
            keep = (row16 >= 3 * k) & (row16 < 3 * k + 3) | (row16 == 12 + k)
            found.append(keep)
        return found

    kept_rows = masks()

    def prepare(turn, halo):
        fulls = [sides(turn, GT + t, True) for t in range(tiles)]
        for copy in halo:
            copy.wait_recv()
        for u in list(range(GT)) + list(range(GT + tiles, 2 * GT + tiles)):
            sides(turn, u, False)
        return fulls

    def nonbonded(turn, fulls, finish, chosen):
        base = spot * tiles - GT
        count = total * tiles
        for t in chosen:
            near = [
                jnp.minimum(lax.rem(nbr_s[j, tiles * block + t] - base + count, count), tiles + 2 * GT - 1)
                for j in range(NBR)
            ]
            a = jnp.concatenate([a_side[u] for u in near], axis=0)
            g = [g_side[u] for u in near]
            g = jnp.concatenate([x for x in g for _ in range(2)], axis=1)
            rows = ext[turn, GT + t]
            force = jnp.zeros((16, TILE), F32)
            for kp in range(KEPT // 2):
                pair = []
                for k in (2 * kp, 2 * kp + 1):
                    blocks = [jnp.where(kept_rows[k], x, 0.0) for x in fulls[t]]
                    pair.append(jnp.concatenate(blocks + [jnp.zeros((32, TILE), F32)], axis=0))
                rhs = jnp.concatenate(pair, axis=1).astype(BF16)
                weights = jnp.exp2(mm(a, rhs))
                stack = []
                for j in range(NBR):
                    stack.extend(split2(weights[j * TILE : (j + 1) * TILE]))
                got = mm(g, jnp.concatenate(stack, axis=0))
                got = got[0:16] + got[16:32]
                for k in (2 * kp, 2 * kp + 1):
                    both = lanes(got, k % 2)
                    force = jnp.where((row16 >= 3 * k) & (row16 < 3 * k + 3), rows * both[12:13] - both, force)
            high, low = split2(force * strengths[t])
            finish(t, mm(wide_table, jnp.concatenate([high, high, low], axis=0)))

    def bonded(current, chosen):
        forces = []
        for n, t in enumerate(chosen):
            high, low = split2(jnp.concatenate([lanes(x, n) for x in current], axis=0))
            table = pick[t]
            got = mm(jnp.concatenate([high, low], axis=1), jnp.concatenate([table, table], axis=0))
            stretch = [got[c * BEADS : (c + 1) * BEADS, :TILE] for c in range(3)]
            arms = [got[c * BEADS : (c + 1) * BEADS, TILE:] for c in range(3)]
            swapped = [pltpu.roll(x, APT, 1) for x in arms]
            factor = -bond_stiff * (sum(x * x for x in stretch) - bond_rest)
            bend = -angle_stiff * (sum(x * y for x, y in zip(arms, swapped)) - angle_rest)
            push = jnp.concatenate(
                [jnp.concatenate([factor * x, bend * y], axis=1) for x, y in zip(stretch, swapped)], axis=0
            )
            high, low = split2(push)
            back = drop[t]
            forces.append(mm(jnp.concatenate([high, low], axis=1), jnp.concatenate([back, back], axis=0)))
        return [
            jnp.concatenate([f[c * BEADS : (c + 1) * BEADS] for f in forces], axis=1) for c in range(3)
        ]

    def advance(current, speed):
        moved, fast = [], []
        for c in range(3):
            first = current[c][0:1]
            both = jnp.concatenate([current[c] - first, speed[c]], axis=0)
            high, low = split2(both)
            got = mm(free_table, jnp.concatenate([high, high, low], axis=0))
            moved.append(first + got[:BEADS])
            fast.append(got[BEADS:])
        return moved, fast

    half = 0.5 * time_step / SUBS

    local[2].wait()
    for copy in q_sends:
        copy.wait_recv()
    current = [q_all[c] for c in range(3)]
    halo = start_halo(0, contracted(current))
    halos = list(halo)
    everything = list(range(tiles))
    pushed = bonded(current, everything)
    kicks = [None] * tiles

    def keep(t, kick):
        kicks[t] = kick

    local[3].wait()
    for copy in p_sends:
        copy.wait_recv()
    fulls = prepare(0, halo)
    ended = []
    for first in range(0, tiles, GROUP):
        chosen = everything[first : first + GROUP]
        span = slice(first * TILE, (first + GROUP) * TILE)
        nonbonded(0, fulls, keep, chosen)
        kick = jnp.concatenate([kicks[t] for t in chosen], axis=1)
        inv = inverse[:, span]
        here = [x[:, span] for x in current]
        speed = [
            (p_all[c, :, span] + half * pushed[c][:, span] + kick[c * BEADS : (c + 1) * BEADS]) * inv for c in range(3)
        ]
        for substep in range(SUBS):
            here, speed = advance(here, speed)
            if substep + 1 < SUBS:
                force = bonded(here, chosen)
                speed = [speed[c] + (2.0 * half) * force[c] * inv for c in range(3)]
        ended.append((here, speed))
    current = [jnp.concatenate([e[0][c] for e in ended], axis=1) for c in range(3)]
    speed = [jnp.concatenate([e[1][c] for e in ended], axis=1) for c in range(3)]

    halo = start_halo(1, contracted(current))
    halos = halos + list(halo)
    for c in range(3):
        q_done[c] = current[c]
    sends = sends + exchange(2, rows_of(q_done), q_out.at[:, :, my_lanes])
    mine_q = pltpu.make_async_copy(q_done.at[:, my_rows, :], q_out.at[:, :, my_lanes], own_sem.at[0])
    mine_q.start()
    pushed = bonded(current, everything)
    moment = [speed[c] * mass_row + half * pushed[c] for c in range(3)]
    late = []

    def send_home(t, kick):
        spans = slice(t * TILE, (t + 1) * TILE)
        for c in range(3):
            p_done[c, :, spans] = lanes(moment[c], t) + kick[c * BEADS : (c + 1) * BEADS]
        if (t + 1) % CHUNK:
            return
        width = CHUNK * TILE
        begin = (t + 1 - CHUNK) * TILE
        here = pl.ds(pl.multiple_of(own * block + begin, TILE), width)
        target = p_out.at[:, :, here]
        for n in order:
            rows = pl.ds(pl.multiple_of(held * peers[n], held), held)
            copy = pltpu.make_async_remote_copy(
                src_ref=p_done.at[:, rows, begin : begin + width],
                dst_ref=target,
                send_sem=send_sem.at[3 + t // CHUNK, n],
                recv_sem=recv_sem.at[3 + t // CHUNK, n],
                device_id=(space, peers[n]),
                device_id_type=MESH,
            )
            copy.start()
            late.append(copy)
        mine = pltpu.make_async_copy(p_done.at[:, my_rows, begin : begin + width], target, own_sem.at[1 + t // CHUNK])
        mine.start()
        late.append(mine)

    nonbonded(1, prepare(1, halo), send_home, everything)
    for copy in sends:
        copy.wait_send()
    for copy in halos:
        copy.wait_send()
    for copy in sends[(2) * (beads - 1) :]:
        copy.wait_recv()
    mine_q.wait()
    for copy in late:
        copy.wait()


def put_out(q_ref, p_ref, q_out, p_out, sem):
    copies = [
        pltpu.make_async_copy(a, b, sem.at[n]) for n, (a, b) in enumerate(((q_ref, q_out), (p_ref, p_out)))
    ]
    for copy in copies:
        copy.start()
    for copy in copies:
        copy.wait()


def solution(mesh):
    spaces, beads = mesh.shape["space"], mesh.shape["bead"]
    table = constant_table()

    def body(positions, momenta, masses, strengths, bond_ends, angle_ends, neighbour_tiles):
        held, _, slab = positions.shape
        own = slab // beads
        tiles = own // TILE
        near = tiles + 2 * GT
        moved = pltpu.VMEM((3, held, slab), F32)
        anywhere = pl.BlockSpec(memory_space=pl.ANY)
        done = pl.pallas_call(
            functools.partial(kernel, spaces, beads),
            out_shape=(moved, moved),
            in_specs=[anywhere] * 8,
            out_specs=(pl.BlockSpec(memory_space=pltpu.VMEM),) * 2,
            scratch_shapes=[
                pltpu.VMEM((3, held, slab), F32),
                pltpu.VMEM((3, held, slab), F32),
                pltpu.VMEM((3, BEADS, own), F32),
                pltpu.VMEM((3, BEADS, own), F32),
                pltpu.VMEM((3, BEADS, own), F32),
                pltpu.VMEM((3, BEADS, own), F32),
                pltpu.VMEM((slab // TILE, TILE), F32),
                pltpu.VMEM((slab // TILE, TILE), F32),
                pltpu.VMEM((2, own), jnp.int32),
                pltpu.VMEM((3, own // 2), jnp.int32),
                pltpu.SMEM((NBR, slab // TILE), jnp.int32),
                pltpu.VMEM(table.shape, BF16),
                pltpu.VMEM((tiles, TILE, 2 * TILE), BF16),
                pltpu.VMEM((tiles, 2 * TILE, TILE), BF16),
                pltpu.VMEM((2, near, 16, TILE), F32),
                pltpu.VMEM((near, TILE, TILE), BF16),
                pltpu.VMEM((near, 32, TILE), BF16),
                pltpu.SemaphoreType.DMA((10,)),
                pltpu.SemaphoreType.DMA((3 + tiles, beads - 1)),
                pltpu.SemaphoreType.DMA((3 + tiles, beads - 1)),
                pltpu.SemaphoreType.DMA((1 + tiles,)),
                pltpu.SemaphoreType.DMA((2, 2)),
                pltpu.SemaphoreType.DMA((2, 2)),
            ],
            compiler_params=pltpu.CompilerParams(collective_id=0, has_side_effects=True),
        )(
            jnp.transpose(positions, (1, 0, 2)),
            jnp.transpose(momenta, (1, 0, 2)),
            masses.reshape(-1, TILE),
            strengths.reshape(-1, TILE),
            bond_ends,
            angle_ends,
            neighbour_tiles,
            jnp.asarray(table),
        )
        done = [pltpu.with_memory_space_constraint(x, pltpu.VMEM) for x in done]
        plain = jax.ShapeDtypeStruct((3, held, slab), F32)
        done = pl.pallas_call(
            put_out,
            out_shape=(plain, plain),
            in_specs=[anywhere] * 2,
            out_specs=(anywhere, anywhere),
            scratch_shapes=[pltpu.SemaphoreType.DMA((2,))],
        )(*done)
        return tuple(jnp.transpose(x, (1, 0, 2)) for x in done)

    placed = (
        P("bead", None, "space"),
        P("bead", None, "space"),
        P("space"),
        P("space"),
        P(None, "space"),
        P(None, "space"),
        P(None, "space"),
    )
    return jax.shard_map(
        body,
        mesh=mesh,
        in_specs=placed,
        out_specs=(P("bead", None, "space"), P("bead", None, "space")),
        check_vma=False,
    )
```

```python
import functools
import math

import jax
import jax.numpy as jnp
import ml_dtypes
import numpy as np
from jax import lax
from jax.experimental import pallas as pl
from jax.experimental.pallas import tpu as pltpu
from jax.sharding import PartitionSpec as P

BEADS = 32
KEPT = 4
SUBS = 3
TILE = 128
GT = 2
NBR = 3
BPT = 128
APT = 64

time_step = 0.3
spring_freq = 80.0
bond_stiff = 0.2
bond_rest = 1.0
angle_stiff = 0.1
angle_rest = 0.5
range_sq = 4.0
CHUNK = 2

F32 = jnp.float32
BF16 = jnp.bfloat16
MESH = pl.DeviceIdType.MESH


def mode_table(number):
    within = np.arange(number)
    result = np.zeros((number, number))
    for column in range(number):
        if column == 0:
            result[:, column] = 1.0 / math.sqrt(number)
        elif 2 * column < number:
            result[:, column] = math.sqrt(2.0 / number) * np.cos(2 * np.pi * within * column / number)
        elif 2 * column == number:
            result[:, column] = (-1.0) ** within / math.sqrt(number)
        else:
            result[:, column] = math.sqrt(2.0 / number) * np.sin(2 * np.pi * within * column / number)
    return result


def contract_table(number, kept):
    larger = mode_table(number)
    smaller = mode_table(kept)
    chosen = [column if 2 * column <= kept else number - kept + column for column in range(kept)]
    return math.sqrt(kept / number) * smaller @ larger[:, chosen].T


def halves(table):
    high = table.astype(ml_dtypes.bfloat16)
    low = (table - high.astype(np.float64)).astype(ml_dtypes.bfloat16)
    return high, low


def three_products(table):
    high, low = halves(table)
    return np.concatenate([high, low, high], axis=1)


def stacked_rows(table):
    high, low = halves(table)
    return np.block([[high, high], [low, low]])


def constant_table():
    modes = mode_table(BEADS)
    interval = time_step / SUBS
    freqs = 2.0 * spring_freq * np.sin(np.pi * np.arange(BEADS) / BEADS)
    safe = np.where(freqs > 0, freqs, 1.0)
    cosine = np.cos(freqs * interval)
    gains = np.where(freqs > 0, np.sin(freqs * interval) / safe, interval)
    drags = freqs * np.sin(freqs * interval)
    keep = (modes * cosine) @ modes.T
    gain = (modes * gains) @ modes.T
    drag = -(modes * drags) @ modes.T
    free = np.block([[keep, gain], [drag, keep]])
    contract = contract_table(BEADS, KEPT)
    narrow = np.zeros((16, 3 * BEADS))
    for k in range(KEPT):
        for c in range(3):
            narrow[3 * k + c, c * BEADS : (c + 1) * BEADS] = contract[k]
    expand = BEADS / KEPT * contract.T
    wide = np.zeros((3 * BEADS, 16))
    for k in range(KEPT):
        for c in range(3):
            wide[c * BEADS : (c + 1) * BEADS, 3 * k + c] = expand[:, k]
    wide *= 0.5 * time_step * 2.0 / range_sq
    table = np.zeros((352, 256), ml_dtypes.bfloat16)
    table[:128, :128] = stacked_rows(free)
    for c in range(3):
        near = narrow[:, c * BEADS : (c + 1) * BEADS] @ free[:BEADS]
        table[128 + 32 * c : 160 + 32 * c, :128] = stacked_rows(near)
    table[224:256, :192] = stacked_rows(narrow)
    table[256:352, :48] = three_products(wide)
    return table


def split2(x):
    high = x.astype(BF16)
    return high, (x - high.astype(F32)).astype(BF16)


def split3(x):
    high = x.astype(BF16)
    rest = x - high.astype(F32)
    middle = rest.astype(BF16)
    return high, middle, (rest - middle.astype(F32)).astype(BF16)


def mm(a, b):
    return jnp.dot(a, b, preferred_element_type=F32)


def lanes(x, t):
    return x[:, t * TILE : (t + 1) * TILE]


def walk(space, place, beads):
    core = lax.rem(space, 2)
    return core * (beads - 1) + (1 - 2 * core) * place


def flip(space):
    return 1 - lax.rem(lax.div(space, 2), 2)


def block_of(space, bead, beads):
    row = lax.div(bead, 2)
    return walk(space, 2 * row + lax.rem(bead + row + flip(space), 2), beads)


def device_of(spot, beads):
    space = lax.div(spot, beads)
    place = walk(space, lax.rem(spot, beads), beads)
    row = lax.div(place, 2)
    return space, 2 * row + lax.rem(place + row + flip(space), 2)


def kernel(
    spaces,
    beads,
    q_in,
    p_in,
    mass_in,
    strength_in,
    bond_in,
    angle_in,
    nbr_in,
    const_in,
    q_out,
    p_out,
    q_stage,
    p_stage,
    q_all,
    p_all,
    q_done,
    p_done,
    mass_v,
    strength_v,
    bond_v,
    angle_v,
    nbr_s,
    const_v,
    pick,
    drop,
    ext,
    a_side,
    g_side,
    own_side,
    local_sem,
    send_sem,
    recv_sem,
    own_sem,
    halo_send,
    halo_recv,
):
    space = lax.axis_index("space")
    me = lax.axis_index("bead")
    slab = q_in.shape[2]
    own = slab // beads
    tiles = own // TILE
    held = q_in.shape[1]
    total = spaces * beads
    block = block_of(space, me, beads)
    spot = space * beads + block
    after_id = device_of(lax.rem(spot + 1, total), beads)
    before_id = device_of(lax.rem(spot + total - 1, total), beads)
    peers = [lax.rem(me + d, beads) for d in range(1, beads)]
    order = sorted(range(beads - 1), key=lambda n: -min(n + 1, beads - n - 1))

    early = pltpu.make_async_copy(q_in, q_stage, local_sem.at[0])
    early.start()
    barrier = pltpu.get_barrier_semaphore()
    for peer in peers:
        pl.semaphore_signal(barrier, inc=1, device_id=(space, peer), device_id_type=MESH)
    for device in (before_id, after_id):
        pl.semaphore_signal(barrier, inc=1, device_id=device, device_id_type=MESH)

    my_rows = pl.ds(pl.multiple_of(held * me, held), held)
    my_lanes = pl.ds(pl.multiple_of(own * block, own), own)
    local = [
        (q_in, q_stage),
        (p_in, p_stage),
        (q_in.at[:, :, my_lanes], q_all.at[:, my_rows, :]),
        (p_in.at[:, :, my_lanes], p_all.at[:, my_rows, :]),
        (bond_in.at[:, my_lanes], bond_v),
        (angle_in.at[:, pl.ds(pl.multiple_of((own // 2) * block, own // 2), own // 2)], angle_v),
        (mass_in, mass_v),
        (strength_in, strength_v),
        (nbr_in, nbr_s),
        (const_in, const_v),
    ]
    local = [pltpu.make_async_copy(a, b, local_sem.at[n]) for n, (a, b) in enumerate(local)]
    for copy in local[1:]:
        copy.start()

    def exchange(kind, source, target):
        copies = []
        for n in order:
            peer = peers[n]
            copies.append(
                pltpu.make_async_remote_copy(
                    src_ref=source(peer),
                    dst_ref=target,
                    send_sem=send_sem.at[kind, n],
                    recv_sem=recv_sem.at[kind, n],
                    device_id=(space, peer),
                    device_id_type=MESH,
                )
            )
        for copy in copies:
            copy.start()
        return copies

    def lanes_of(ref):
        return lambda peer: ref.at[:, :, pl.ds(pl.multiple_of(own * block_of(space, peer, beads), own), own)]

    def rows_of(ref):
        return lambda peer: ref.at[:, pl.ds(pl.multiple_of(held * peer, held), held), :]

    pl.semaphore_wait(barrier, beads + 1)
    local[0].wait()
    sends = exchange(0, lanes_of(q_stage), q_all.at[:, my_rows, :])
    q_sends = list(sends)
    local[1].wait()
    p_sends = exchange(1, lanes_of(p_stage), p_all.at[:, my_rows, :])
    sends = sends + p_sends

    for n in (4, 5, 6, 7, 8, 9):
        local[n].wait()

    place = lax.broadcasted_iota(jnp.int32, (TILE, TILE), 0)
    lane = lax.broadcasted_iota(jnp.int32, (8, TILE), 1)

    def hot(row):
        return jnp.where(place == row, 1.0, 0.0).astype(F32)

    for t in range(tiles):
        ends = bond_v[:, t * TILE : (t + 1) * TILE]
        bonds = hot(ends[0:1]) - hot(ends[1:2])
        pair = angle_v[:, (t // 2) * TILE : (t // 2 + 1) * TILE]
        rows = [jnp.broadcast_to(pair[e : e + 1], (8, TILE)) for e in range(3)]
        turned = [pltpu.roll(r, APT, 1) for r in rows]
        left, right = (rows, turned) if t % 2 == 0 else (turned, rows)
        outer = jnp.where(lane < APT, left[0], right[2])[0:1]
        centre = jnp.where(lane < APT, left[1], right[1])[0:1]
        angles = hot(outer) - hot(centre)
        pick[t] = jnp.concatenate([bonds, angles], axis=1).astype(BF16)
        drop[t] = jnp.concatenate([jnp.transpose(bonds), jnp.transpose(angles)], axis=0).astype(BF16)

    mass_row = jnp.concatenate([mass_v[pl.ds(tiles * block + t, 1), :] for t in range(tiles)], axis=1)
    inverse = 1.0 / mass_row
    strengths = [strength_v[pl.ds(tiles * block + t, 1), :] for t in range(tiles)]

    free_rows = const_v[0:128, 0:128]
    near_rows = [const_v[128 + 32 * c : 160 + 32 * c, 0:128] for c in range(3)]
    narrow_rows = const_v[224:256, 0:192]
    wide_table = const_v[256:352, 0:48]

    row16 = lax.broadcasted_iota(jnp.int32, (16, TILE), 0)
    feature = row16 < 12
    row_wide = lax.broadcasted_iota(jnp.int32, (16, own), 0)

    def contracted(current):
        high, low = split2(jnp.concatenate(current, axis=0))
        got = mm(narrow_rows, jnp.concatenate([high, low], axis=0))
        return got[:16] + got[16:]

    def start_halo(turn, narrow):
        for t in range(tiles):
            ext[turn, GT + t] = jnp.where(feature, lanes(narrow, t), strengths[t])
        copies = []
        for side, device, source, target in (
            (0, before_id, GT, GT + tiles),
            (1, after_id, tiles, 0),
        ):
            copies.append(
                pltpu.make_async_remote_copy(
                    src_ref=ext.at[turn, pl.ds(source, GT)],
                    dst_ref=ext.at[turn, pl.ds(target, GT)],
                    send_sem=halo_send.at[turn, side],
                    recv_sem=halo_recv.at[turn, side],
                    device_id=device,
                    device_id_type=MESH,
                )
            )
        for copy in copies:
            copy.start()
        return copies

    scale = math.sqrt(2.0 / range_sq * math.log2(math.e))

    def sides(turn, u, with_own):
        rows = ext[turn, u]
        scaled = rows * scale
        square = scaled * scaled
        norms = scaled
        for k in range(KEPT):
            part = 0.5 * (square[3 * k : 3 * k + 1] + square[3 * k + 1 : 3 * k + 2] + square[3 * k + 2 : 3 * k + 3])
            norms = jnp.where(row16 == 12 + k, part, norms)
        parts = split3(norms)
        wide_parts = [x.astype(F32) for x in parts]
        ones = [jnp.where(feature, x, 1.0) for x in wide_parts]
        stack = jnp.concatenate(
            [wide_parts[0], wide_parts[1], ones[0], ones[1], wide_parts[2], ones[0], jnp.zeros((32, TILE), F32)], axis=0
        )
        a_side[u] = jnp.transpose(stack).astype(BF16)
        weight = rows[12:13]
        g_high, g_low = split2(jnp.where(feature, rows * weight, weight))
        g_side[u] = jnp.concatenate([g_high, g_low], axis=0)
        if not with_own:
            return None
        h, m, l = wide_parts

        def own_block(left, right):
            return jnp.where(feature, left, right)

        minus = -jnp.ones_like(h)

        def shift(x):
            return -x

        full = [
            own_block(h, minus),
            own_block(h, minus),
            own_block(m, shift(h)),
            own_block(m, shift(m)),
            own_block(h, minus),
            own_block(l, shift(l)),
        ]
        return full

    def masks():
        found = []
        for k in range(KEPT):
            keep = (row16 >= 3 * k) & (row16 < 3 * k + 3) | (row16 == 12 + k)
            found.append(keep)
        return found

    kept_rows = masks()

    def prepare(turn, halo):
        for t in range(tiles):
            full = sides(turn, GT + t, True)
            parts = []
            for k in range(KEPT):
                blocks = [jnp.where(kept_rows[k], x, 0.0) for x in full]
                parts.append(jnp.concatenate(blocks + [jnp.zeros((32, TILE), F32)], axis=0))
            own_side[t] = jnp.concatenate(parts, axis=1).astype(BF16)
        for copy in halo:
            copy.wait_recv()
        for u in list(range(GT)) + list(range(GT + tiles, 2 * GT + tiles)):
            sides(turn, u, False)

    def nonbonded(turn, finish, chunk):
        base = spot * tiles - GT
        count = total * tiles
        found = []
        for t in range(tiles):
            near = [
                jnp.minimum(lax.rem(nbr_s[j, tiles * block + t] - base + count, count), tiles + 2 * GT - 1)
                for j in range(NBR)
            ]
            a = jnp.concatenate([a_side[u] for u in near], axis=0)
            g = [g_side[u] for u in near]
            g = jnp.concatenate([x for x in g for _ in range(2)], axis=1)
            rows = ext[turn, GT + t]
            weights = jnp.exp2(mm(a, own_side[t]))
            stack = []
            for j in range(NBR):
                stack.extend(split2(weights[j * TILE : (j + 1) * TILE]))
            got = mm(g, jnp.concatenate(stack, axis=0))
            got = got[0:16] + got[16:32]
            force = jnp.zeros((16, TILE), F32)
            for k in range(KEPT):
                both = lanes(got, k)
                force = jnp.where((row16 >= 3 * k) & (row16 < 3 * k + 3), rows * both[12:13] - both, force)
            found.append(force * strengths[t])
            if len(found) == chunk:
                high, low = split2(jnp.concatenate(found, axis=1))
                found = []
                finish(t, mm(wide_table, jnp.concatenate([high, high, low], axis=0)))

    def bonded(current, chosen):
        forces = []
        for n, t in enumerate(chosen):
            high, low = split2(jnp.concatenate([lanes(x, n) for x in current], axis=0))
            table = pick[t]
            got = mm(jnp.concatenate([high, low], axis=0), table)
            got = got[: 3 * BEADS] + got[3 * BEADS :]
            stretch = [got[c * BEADS : (c + 1) * BEADS, :TILE] for c in range(3)]
            arms = [got[c * BEADS : (c + 1) * BEADS, TILE:] for c in range(3)]
            swapped = [pltpu.roll(x, APT, 1) for x in arms]
            factor = -bond_stiff * (sum(x * x for x in stretch) - bond_rest)
            bend = -angle_stiff * (sum(x * y for x, y in zip(arms, swapped)) - angle_rest)
            push = jnp.concatenate(
                [jnp.concatenate([factor * x, bend * y], axis=1) for x, y in zip(stretch, swapped)], axis=0
            )
            high, low = split2(push)
            back = drop[t]
            got = mm(jnp.concatenate([high, low], axis=0), back)
            forces.append(got[: 3 * BEADS] + got[3 * BEADS :])
        return [
            jnp.concatenate([f[c * BEADS : (c + 1) * BEADS] for f in forces], axis=1) for c in range(3)
        ]

    def advance(current, speed, last=False):
        moved, fast = [], []
        narrow = None
        for c in range(3):
            first = current[c][0:1]
            both = jnp.concatenate([current[c] - first, speed[c]], axis=0)
            high, low = split2(both)
            table = jnp.concatenate([free_rows, near_rows[c]], axis=0) if last else free_rows
            got = mm(table, jnp.concatenate([high, low], axis=0))
            if last:
                part = got[4 * BEADS : 4 * BEADS + 16] + got[4 * BEADS + 16 :]
                part = part + jnp.where(lax.rem(row_wide, 3) == c, first, 0.0)
                narrow = part if narrow is None else narrow + part
            got = got[: 2 * BEADS] + got[2 * BEADS : 4 * BEADS]
            moved.append(first + got[:BEADS])
            fast.append(got[BEADS:])
        return moved, fast, narrow

    half = 0.5 * time_step / SUBS

    local[2].wait()
    for copy in q_sends:
        copy.wait_recv()
    current = [q_all[c] for c in range(3)]
    halo = start_halo(0, contracted(current))
    halos = list(halo)
    everything = list(range(tiles))
    pushed = bonded(current, everything)
    kicks = []

    def keep(t, kick):
        kicks.append(kick)

    local[3].wait()
    for copy in p_sends:
        copy.wait_recv()
    prepare(0, halo)
    nonbonded(0, keep, tiles)
    kick = kicks[0]
    speed = [
        (p_all[c] + half * pushed[c] + kick[c * BEADS : (c + 1) * BEADS]) * inverse for c in range(3)
    ]
    for substep in range(SUBS - 1):
        current, speed, _ = advance(current, speed)
        force = bonded(current, everything)
        speed = [speed[c] + (2.0 * half) * force[c] * inverse for c in range(3)]
    current, speed, narrow = advance(current, speed, True)
    halo = start_halo(1, narrow)
    halos = halos + list(halo)
    for c in range(3):
        q_done[c] = current[c]
    sends = sends + exchange(2, rows_of(q_done), q_out.at[:, :, my_lanes])
    mine_q = pltpu.make_async_copy(q_done.at[:, my_rows, :], q_out.at[:, :, my_lanes], own_sem.at[0])
    mine_q.start()
    pushed = bonded(current, everything)
    moment = [speed[c] * mass_row + half * pushed[c] for c in range(3)]
    late = []

    def send_home(t, kick):
        width = CHUNK * TILE
        begin = (t + 1 - CHUNK) * TILE
        for c in range(3):
            p_done[c, :, begin : begin + width] = (
                moment[c][:, begin : begin + width] + kick[c * BEADS : (c + 1) * BEADS]
            )
        here = pl.ds(pl.multiple_of(own * block + begin, TILE), width)
        target = p_out.at[:, :, here]
        for n in order:
            rows = pl.ds(pl.multiple_of(held * peers[n], held), held)
            copy = pltpu.make_async_remote_copy(
                src_ref=p_done.at[:, rows, begin : begin + width],
                dst_ref=target,
                send_sem=send_sem.at[3 + t // CHUNK, n],
                recv_sem=recv_sem.at[3 + t // CHUNK, n],
                device_id=(space, peers[n]),
                device_id_type=MESH,
            )
            copy.start()
            late.append(copy)
        mine = pltpu.make_async_copy(p_done.at[:, my_rows, begin : begin + width], target, own_sem.at[1 + t // CHUNK])
        mine.start()
        late.append(mine)

    prepare(1, halo)
    nonbonded(1, send_home, CHUNK)
    for copy in sends:
        copy.wait_send()
    for copy in halos:
        copy.wait_send()
    for copy in sends[(2) * (beads - 1) :]:
        copy.wait_recv()
    mine_q.wait()
    for copy in late:
        copy.wait()


def put_out(q_ref, p_ref, q_out, p_out, sem):
    copies = [
        pltpu.make_async_copy(a, b, sem.at[n]) for n, (a, b) in enumerate(((q_ref, q_out), (p_ref, p_out)))
    ]
    for copy in copies:
        copy.start()
    for copy in copies:
        copy.wait()


def solution(mesh):
    spaces, beads = mesh.shape["space"], mesh.shape["bead"]
    table = constant_table()

    def body(positions, momenta, masses, strengths, bond_ends, angle_ends, neighbour_tiles):
        held, _, slab = positions.shape
        own = slab // beads
        tiles = own // TILE
        near = tiles + 2 * GT
        moved = pltpu.VMEM((3, held, slab), F32)
        anywhere = pl.BlockSpec(memory_space=pl.ANY)
        done = pl.pallas_call(
            functools.partial(kernel, spaces, beads),
            out_shape=(moved, moved),
            in_specs=[anywhere] * 8,
            out_specs=(pl.BlockSpec(memory_space=pltpu.VMEM),) * 2,
            scratch_shapes=[
                pltpu.VMEM((3, held, slab), F32),
                pltpu.VMEM((3, held, slab), F32),
                pltpu.VMEM((3, BEADS, own), F32),
                pltpu.VMEM((3, BEADS, own), F32),
                pltpu.VMEM((3, BEADS, own), F32),
                pltpu.VMEM((3, BEADS, own), F32),
                pltpu.VMEM((slab // TILE, TILE), F32),
                pltpu.VMEM((slab // TILE, TILE), F32),
                pltpu.VMEM((2, own), jnp.int32),
                pltpu.VMEM((3, own // 2), jnp.int32),
                pltpu.SMEM((NBR, slab // TILE), jnp.int32),
                pltpu.VMEM(table.shape, BF16),
                pltpu.VMEM((tiles, TILE, 2 * TILE), BF16),
                pltpu.VMEM((tiles, 2 * TILE, TILE), BF16),
                pltpu.VMEM((2, near, 16, TILE), F32),
                pltpu.VMEM((near, TILE, TILE), BF16),
                pltpu.VMEM((near, 32, TILE), BF16),
                pltpu.VMEM((tiles, TILE, KEPT * TILE), BF16),
                pltpu.SemaphoreType.DMA((10,)),
                pltpu.SemaphoreType.DMA((3 + tiles, beads - 1)),
                pltpu.SemaphoreType.DMA((3 + tiles, beads - 1)),
                pltpu.SemaphoreType.DMA((1 + tiles,)),
                pltpu.SemaphoreType.DMA((2, 2)),
                pltpu.SemaphoreType.DMA((2, 2)),
            ],
            compiler_params=pltpu.CompilerParams(collective_id=0, has_side_effects=True),
        )(
            jnp.transpose(positions, (1, 0, 2)),
            jnp.transpose(momenta, (1, 0, 2)),
            masses.reshape(-1, TILE),
            strengths.reshape(-1, TILE),
            bond_ends,
            angle_ends,
            neighbour_tiles,
            jnp.asarray(table),
        )
        done = [pltpu.with_memory_space_constraint(x, pltpu.VMEM) for x in done]
        plain = jax.ShapeDtypeStruct((3, held, slab), F32)
        done = pl.pallas_call(
            put_out,
            out_shape=(plain, plain),
            in_specs=[anywhere] * 2,
            out_specs=(anywhere, anywhere),
            scratch_shapes=[pltpu.SemaphoreType.DMA((2,))],
        )(*done)
        return tuple(jnp.transpose(x, (1, 0, 2)) for x in done)

    placed = (
        P("bead", None, "space"),
        P("bead", None, "space"),
        P("space"),
        P("space"),
        P(None, "space"),
        P(None, "space"),
        P(None, "space"),
    )
    return jax.shard_map(
        body,
        mesh=mesh,
        in_specs=placed,
        out_specs=(P("bead", None, "space"), P("bead", None, "space")),
        check_vma=False,
    )
```

```python
import functools
import math

import jax
import jax.numpy as jnp
import ml_dtypes
import numpy as np
from jax import lax
from jax.experimental import pallas as pl
from jax.experimental.pallas import tpu as pltpu
from jax.sharding import PartitionSpec as P

BEADS = 32
KEPT = 4
SUBS = 3
TILE = 128
GT = 2
NBR = 3
BPT = 128
APT = 64

time_step = 0.3
spring_freq = 80.0
bond_stiff = 0.2
bond_rest = 1.0
angle_stiff = 0.1
angle_rest = 0.5
range_sq = 4.0
CHUNK = 2

F32 = jnp.float32
BF16 = jnp.bfloat16
MESH = pl.DeviceIdType.MESH


def mode_table(number):
    within = np.arange(number)
    result = np.zeros((number, number))
    for column in range(number):
        if column == 0:
            result[:, column] = 1.0 / math.sqrt(number)
        elif 2 * column < number:
            result[:, column] = math.sqrt(2.0 / number) * np.cos(2 * np.pi * within * column / number)
        elif 2 * column == number:
            result[:, column] = (-1.0) ** within / math.sqrt(number)
        else:
            result[:, column] = math.sqrt(2.0 / number) * np.sin(2 * np.pi * within * column / number)
    return result


def contract_table(number, kept):
    larger = mode_table(number)
    smaller = mode_table(kept)
    chosen = [column if 2 * column <= kept else number - kept + column for column in range(kept)]
    return math.sqrt(kept / number) * smaller @ larger[:, chosen].T


def halves(table):
    high = table.astype(ml_dtypes.bfloat16)
    low = (table - high.astype(np.float64)).astype(ml_dtypes.bfloat16)
    return high, low


def three_products(table):
    high, low = halves(table)
    return np.concatenate([high, low, high], axis=1)


def stacked_rows(table):
    high, low = halves(table)
    return np.block([[high, high], [low, low]])


def constant_table():
    modes = mode_table(BEADS)
    interval = time_step / SUBS
    freqs = 2.0 * spring_freq * np.sin(np.pi * np.arange(BEADS) / BEADS)
    safe = np.where(freqs > 0, freqs, 1.0)
    cosine = np.cos(freqs * interval)
    gains = np.where(freqs > 0, np.sin(freqs * interval) / safe, interval)
    drags = freqs * np.sin(freqs * interval)
    keep = (modes * cosine) @ modes.T
    gain = (modes * gains) @ modes.T
    drag = -(modes * drags) @ modes.T
    free = np.block([[keep, gain], [drag, keep]])
    contract = contract_table(BEADS, KEPT)
    narrow = np.zeros((16, 3 * BEADS))
    for k in range(KEPT):
        for c in range(3):
            narrow[3 * k + c, c * BEADS : (c + 1) * BEADS] = contract[k]
    expand = BEADS / KEPT * contract.T
    wide = np.zeros((3 * BEADS, 16))
    for k in range(KEPT):
        for c in range(3):
            wide[c * BEADS : (c + 1) * BEADS, 3 * k + c] = expand[:, k]
    wide *= 0.5 * time_step * 2.0 / range_sq
    table = np.zeros((352, 256), ml_dtypes.bfloat16)
    table[:128, :128] = stacked_rows(free)
    for c in range(3):
        near = narrow[:, c * BEADS : (c + 1) * BEADS] @ free[:BEADS]
        table[128 + 32 * c : 160 + 32 * c, :128] = stacked_rows(near)
    table[224:256, :192] = stacked_rows(narrow)
    table[256:352, :48] = three_products(wide)
    return table


def split2(x):
    high = x.astype(BF16)
    return high, (x - high.astype(F32)).astype(BF16)


def split3(x):
    high = x.astype(BF16)
    rest = x - high.astype(F32)
    middle = rest.astype(BF16)
    return high, middle, (rest - middle.astype(F32)).astype(BF16)


def mm(a, b):
    return jnp.dot(a, b, preferred_element_type=F32)


def lanes(x, t):
    return x[:, t * TILE : (t + 1) * TILE]


def walk(space, place, beads):
    core = lax.rem(space, 2)
    return core * (beads - 1) + (1 - 2 * core) * place


def flip(space):
    return 1 - lax.rem(lax.div(space, 2), 2)


def block_of(space, bead, beads):
    row = lax.div(bead, 2)
    return walk(space, 2 * row + lax.rem(bead + row + flip(space), 2), beads)


def device_of(spot, beads):
    space = lax.div(spot, beads)
    place = walk(space, lax.rem(spot, beads), beads)
    row = lax.div(place, 2)
    return space, 2 * row + lax.rem(place + row + flip(space), 2)


def kernel(
    spaces,
    beads,
    q_in,
    p_in,
    mass_in,
    strength_in,
    bond_in,
    angle_in,
    nbr_in,
    const_in,
    q_out,
    p_out,
    q_stage,
    p_stage,
    q_all,
    p_all,
    q_done,
    p_done,
    mass_v,
    strength_v,
    bond_v,
    angle_v,
    nbr_s,
    const_v,
    pick,
    drop,
    ext,
    a_side,
    g_side,
    own_side,
    local_sem,
    send_sem,
    recv_sem,
    own_sem,
    halo_send,
    halo_recv,
):
    space = lax.axis_index("space")
    me = lax.axis_index("bead")
    slab = q_in.shape[2]
    own = slab // beads
    tiles = own // TILE
    held = q_in.shape[1]
    total = spaces * beads
    block = block_of(space, me, beads)
    spot = space * beads + block
    after_id = device_of(lax.rem(spot + 1, total), beads)
    before_id = device_of(lax.rem(spot + total - 1, total), beads)
    peers = [lax.rem(me + d, beads) for d in range(1, beads)]
    order = sorted(range(beads - 1), key=lambda n: -min(n + 1, beads - n - 1))

    early = pltpu.make_async_copy(q_in, q_stage, local_sem.at[0])
    early.start()
    barrier = pltpu.get_barrier_semaphore()
    for peer in peers:
        pl.semaphore_signal(barrier, inc=1, device_id=(space, peer), device_id_type=MESH)
    for device in (before_id, after_id):
        pl.semaphore_signal(barrier, inc=1, device_id=device, device_id_type=MESH)

    my_rows = pl.ds(pl.multiple_of(held * me, held), held)
    my_lanes = pl.ds(pl.multiple_of(own * block, own), own)
    local = [
        (q_in, q_stage),
        (p_in, p_stage),
        (q_in.at[:, :, my_lanes], q_all.at[:, my_rows, :]),
        (p_in.at[:, :, my_lanes], p_all.at[:, my_rows, :]),
        (bond_in.at[:, my_lanes], bond_v),
        (angle_in.at[:, pl.ds(pl.multiple_of((own // 2) * block, own // 2), own // 2)], angle_v),
        (mass_in, mass_v),
        (strength_in, strength_v),
        (nbr_in, nbr_s),
        (const_in, const_v),
    ]
    local = [pltpu.make_async_copy(a, b, local_sem.at[n]) for n, (a, b) in enumerate(local)]
    for copy in local[1:]:
        copy.start()

    def exchange(kind, source, target):
        for n in order:
            pltpu.make_async_remote_copy(
                src_ref=source(peers[n]),
                dst_ref=target,
                send_sem=send_sem.at[kind],
                recv_sem=recv_sem.at[kind],
                device_id=(space, peers[n]),
                device_id_type=MESH,
            ).start()

    def wait_all(sem):
        sized = q_stage.at[:, :, pl.ds(0, (beads - 1) * own)]
        pltpu.make_async_copy(sized, sized, sem).wait()

    def lanes_of(ref):
        return lambda peer: ref.at[:, :, pl.ds(pl.multiple_of(own * block_of(space, peer, beads), own), own)]

    def rows_of(ref):
        return lambda peer: ref.at[:, pl.ds(pl.multiple_of(held * peer, held), held), :]

    pl.semaphore_wait(barrier, beads + 1)
    local[0].wait()
    exchange(0, lanes_of(q_stage), q_all.at[:, my_rows, :])
    local[1].wait()
    exchange(1, lanes_of(p_stage), p_all.at[:, my_rows, :])

    for n in (4, 5, 6, 7, 8, 9):
        local[n].wait()

    place = lax.broadcasted_iota(jnp.int32, (TILE, TILE), 0)
    lane = lax.broadcasted_iota(jnp.int32, (8, TILE), 1)

    def hot(row):
        return jnp.where(place == row, 1.0, 0.0).astype(F32)

    for t in range(tiles):
        ends = bond_v[:, t * TILE : (t + 1) * TILE]
        bonds = hot(ends[0:1]) - hot(ends[1:2])
        pair = angle_v[:, (t // 2) * TILE : (t // 2 + 1) * TILE]
        rows = [jnp.broadcast_to(pair[e : e + 1], (8, TILE)) for e in range(3)]
        turned = [pltpu.roll(r, APT, 1) for r in rows]
        left, right = (rows, turned) if t % 2 == 0 else (turned, rows)
        outer = jnp.where(lane < APT, left[0], right[2])[0:1]
        centre = jnp.where(lane < APT, left[1], right[1])[0:1]
        angles = hot(outer) - hot(centre)
        pick[t] = jnp.concatenate([bonds, angles], axis=1).astype(BF16)
        drop[t] = jnp.concatenate([jnp.transpose(bonds), jnp.transpose(angles)], axis=0).astype(BF16)

    mass_row = jnp.concatenate([mass_v[pl.ds(tiles * block + t, 1), :] for t in range(tiles)], axis=1)
    inverse = 1.0 / mass_row
    strengths = [strength_v[pl.ds(tiles * block + t, 1), :] for t in range(tiles)]

    free_rows = const_v[0:128, 0:128]
    near_rows = [const_v[128 + 32 * c : 160 + 32 * c, 0:128] for c in range(3)]
    narrow_rows = const_v[224:256, 0:192]
    wide_table = const_v[256:352, 0:48]

    row16 = lax.broadcasted_iota(jnp.int32, (16, TILE), 0)
    feature = row16 < 12
    row_wide = lax.broadcasted_iota(jnp.int32, (16, own), 0)

    def contracted(current):
        high, low = split2(jnp.concatenate(current, axis=0))
        got = mm(narrow_rows, jnp.concatenate([high, low], axis=0))
        return got[:16] + got[16:]

    def start_halo(turn, narrow):
        for t in range(tiles):
            ext[turn, GT + t] = jnp.where(feature, lanes(narrow, t), strengths[t])
        for device, source, target in ((before_id, GT, GT + tiles), (after_id, tiles, 0)):
            pltpu.make_async_remote_copy(
                src_ref=ext.at[turn, pl.ds(source, GT)],
                dst_ref=ext.at[turn, pl.ds(target, GT)],
                send_sem=halo_send.at[turn],
                recv_sem=halo_recv.at[turn],
                device_id=device,
                device_id_type=MESH,
            ).start()

    def wait_halo(sem):
        both = ext.at[0, pl.ds(0, 2 * GT)]
        pltpu.make_async_copy(both, both, sem).wait()

    scale = math.sqrt(2.0 / range_sq * math.log2(math.e))

    def sides(turn, u, with_own):
        rows = ext[turn, u]
        scaled = rows * scale
        square = scaled * scaled
        norms = scaled
        for k in range(KEPT):
            part = 0.5 * (square[3 * k : 3 * k + 1] + square[3 * k + 1 : 3 * k + 2] + square[3 * k + 2 : 3 * k + 3])
            norms = jnp.where(row16 == 12 + k, part, norms)
        parts = split3(norms)
        wide_parts = [x.astype(F32) for x in parts]
        ones = [jnp.where(feature, x, 1.0) for x in wide_parts]
        stack = jnp.concatenate(
            [wide_parts[0], wide_parts[1], ones[0], ones[1], wide_parts[2], ones[0], jnp.zeros((32, TILE), F32)], axis=0
        )
        a_side[u] = jnp.transpose(stack).astype(BF16)
        weight = rows[12:13]
        g_high, g_low = split2(jnp.where(feature, rows * weight, weight))
        g_side[u] = jnp.concatenate([g_high, g_low], axis=0)
        if not with_own:
            return None
        h, m, l = wide_parts

        def own_block(left, right):
            return jnp.where(feature, left, right)

        minus = -jnp.ones_like(h)

        def shift(x):
            return -x

        full = [
            own_block(h, minus),
            own_block(h, minus),
            own_block(m, shift(h)),
            own_block(m, shift(m)),
            own_block(h, minus),
            own_block(l, shift(l)),
        ]
        return full

    def masks():
        found = []
        for k in range(KEPT):
            keep = (row16 >= 3 * k) & (row16 < 3 * k + 3) | (row16 == 12 + k)
            found.append(keep)
        return found

    kept_rows = masks()

    def prepare(turn):
        for t in range(tiles):
            full = sides(turn, GT + t, True)
            parts = []
            for k in range(KEPT):
                blocks = [jnp.where(kept_rows[k], x, 0.0) for x in full]
                parts.append(jnp.concatenate(blocks + [jnp.zeros((32, TILE), F32)], axis=0))
            own_side[t] = jnp.concatenate(parts, axis=1).astype(BF16)
        wait_halo(halo_recv.at[turn])
        for u in list(range(GT)) + list(range(GT + tiles, 2 * GT + tiles)):
            sides(turn, u, False)

    def nonbonded(turn, finish, chunk):
        base = spot * tiles - GT
        count = total * tiles
        found = []
        for t in range(tiles):
            near = [
                jnp.minimum(lax.rem(nbr_s[j, tiles * block + t] - base + count, count), tiles + 2 * GT - 1)
                for j in range(NBR)
            ]
            a = jnp.concatenate([a_side[u] for u in near], axis=0)
            g = [g_side[u] for u in near]
            g = jnp.concatenate([x for x in g for _ in range(2)], axis=1)
            rows = ext[turn, GT + t]
            weights = jnp.exp2(mm(a, own_side[t]))
            stack = []
            for j in range(NBR):
                stack.extend(split2(weights[j * TILE : (j + 1) * TILE]))
            got = mm(g, jnp.concatenate(stack, axis=0))
            got = got[0:16] + got[16:32]
            force = jnp.zeros((16, TILE), F32)
            for k in range(KEPT):
                both = lanes(got, k)
                force = jnp.where((row16 >= 3 * k) & (row16 < 3 * k + 3), rows * both[12:13] - both, force)
            found.append(force * strengths[t])
            if len(found) == chunk:
                high, low = split2(jnp.concatenate(found, axis=1))
                found = []
                finish(t, mm(wide_table, jnp.concatenate([high, high, low], axis=0)))

    def bonded(current, chosen):
        forces = []
        for n, t in enumerate(chosen):
            high, low = split2(jnp.concatenate([lanes(x, n) for x in current], axis=0))
            table = pick[t]
            got = mm(jnp.concatenate([high, low], axis=0), table)
            got = got[: 3 * BEADS] + got[3 * BEADS :]
            stretch = [got[c * BEADS : (c + 1) * BEADS, :TILE] for c in range(3)]
            arms = [got[c * BEADS : (c + 1) * BEADS, TILE:] for c in range(3)]
            swapped = [pltpu.roll(x, APT, 1) for x in arms]
            factor = -bond_stiff * (sum(x * x for x in stretch) - bond_rest)
            bend = -angle_stiff * (sum(x * y for x, y in zip(arms, swapped)) - angle_rest)
            push = jnp.concatenate(
                [jnp.concatenate([factor * x, bend * y], axis=1) for x, y in zip(stretch, swapped)], axis=0
            )
            high, low = split2(push)
            back = drop[t]
            got = mm(jnp.concatenate([high, low], axis=0), back)
            forces.append(got[: 3 * BEADS] + got[3 * BEADS :])
        return [
            jnp.concatenate([f[c * BEADS : (c + 1) * BEADS] for f in forces], axis=1) for c in range(3)
        ]

    def advance(current, speed, last=False):
        moved, fast = [], []
        narrow = None
        for c in range(3):
            first = current[c][0:1]
            both = jnp.concatenate([current[c] - first, speed[c]], axis=0)
            high, low = split2(both)
            table = jnp.concatenate([free_rows, near_rows[c]], axis=0) if last else free_rows
            got = mm(table, jnp.concatenate([high, low], axis=0))
            if last:
                part = got[4 * BEADS : 4 * BEADS + 16] + got[4 * BEADS + 16 :]
                part = part + jnp.where(lax.rem(row_wide, 3) == c, first, 0.0)
                narrow = part if narrow is None else narrow + part
            got = got[: 2 * BEADS] + got[2 * BEADS : 4 * BEADS]
            moved.append(first + got[:BEADS])
            fast.append(got[BEADS:])
        return moved, fast, narrow

    half = 0.5 * time_step / SUBS

    local[2].wait()
    wait_all(recv_sem.at[0])
    current = [q_all[c] for c in range(3)]
    start_halo(0, contracted(current))
    everything = list(range(tiles))
    pushed = bonded(current, everything)
    kicks = []

    def keep(t, kick):
        kicks.append(kick)

    local[3].wait()
    wait_all(recv_sem.at[1])
    prepare(0)
    nonbonded(0, keep, tiles)
    kick = kicks[0]
    speed = [
        (p_all[c] + half * pushed[c] + kick[c * BEADS : (c + 1) * BEADS]) * inverse for c in range(3)
    ]
    for substep in range(SUBS - 1):
        current, speed, _ = advance(current, speed)
        force = bonded(current, everything)
        speed = [speed[c] + (2.0 * half) * force[c] * inverse for c in range(3)]
    current, speed, narrow = advance(current, speed, True)
    start_halo(1, narrow)
    for c in range(3):
        q_done[c] = current[c]
    exchange(2, rows_of(q_done), q_out.at[:, :, my_lanes])
    mine_q = pltpu.make_async_copy(q_done.at[:, my_rows, :], q_out.at[:, :, my_lanes], own_sem.at[0])
    mine_q.start()
    pushed = bonded(current, everything)
    moment = [speed[c] * mass_row + half * pushed[c] for c in range(3)]
    late = []

    def send_home(t, kick):
        width = CHUNK * TILE
        begin = (t + 1 - CHUNK) * TILE
        for c in range(3):
            p_done[c, :, begin : begin + width] = (
                moment[c][:, begin : begin + width] + kick[c * BEADS : (c + 1) * BEADS]
            )
        here = pl.ds(pl.multiple_of(own * block + begin, TILE), width)
        target = p_out.at[:, :, here]
        for n in order:
            rows = pl.ds(pl.multiple_of(held * peers[n], held), held)
            pltpu.make_async_remote_copy(
                src_ref=p_done.at[:, rows, begin : begin + width],
                dst_ref=target,
                send_sem=send_sem.at[3],
                recv_sem=recv_sem.at[3],
                device_id=(space, peers[n]),
                device_id_type=MESH,
            ).start()
        mine = pltpu.make_async_copy(p_done.at[:, my_rows, begin : begin + width], target, own_sem.at[1 + t // CHUNK])
        mine.start()
        late.append(mine)

    prepare(1)
    nonbonded(1, send_home, CHUNK)
    for kind in range(4):
        wait_all(send_sem.at[kind])
    for turn in range(2):
        wait_halo(halo_send.at[turn])
    wait_all(recv_sem.at[2])
    mine_q.wait()
    for copy in late:
        copy.wait()
    wait_all(recv_sem.at[3])


def put_out(q_ref, p_ref, q_out, p_out, sem):
    copies = [
        pltpu.make_async_copy(a, b, sem.at[n]) for n, (a, b) in enumerate(((q_ref, q_out), (p_ref, p_out)))
    ]
    for copy in copies:
        copy.start()
    for copy in copies:
        copy.wait()


def solution(mesh):
    spaces, beads = mesh.shape["space"], mesh.shape["bead"]
    table = constant_table()

    def body(positions, momenta, masses, strengths, bond_ends, angle_ends, neighbour_tiles):
        held, _, slab = positions.shape
        own = slab // beads
        tiles = own // TILE
        near = tiles + 2 * GT
        moved = pltpu.VMEM((3, held, slab), F32)
        anywhere = pl.BlockSpec(memory_space=pl.ANY)
        done = pl.pallas_call(
            functools.partial(kernel, spaces, beads),
            out_shape=(moved, moved),
            in_specs=[anywhere] * 8,
            out_specs=(pl.BlockSpec(memory_space=pltpu.VMEM),) * 2,
            scratch_shapes=[
                pltpu.VMEM((3, held, slab), F32),
                pltpu.VMEM((3, held, slab), F32),
                pltpu.VMEM((3, BEADS, own), F32),
                pltpu.VMEM((3, BEADS, own), F32),
                pltpu.VMEM((3, BEADS, own), F32),
                pltpu.VMEM((3, BEADS, own), F32),
                pltpu.VMEM((slab // TILE, TILE), F32),
                pltpu.VMEM((slab // TILE, TILE), F32),
                pltpu.VMEM((2, own), jnp.int32),
                pltpu.VMEM((3, own // 2), jnp.int32),
                pltpu.SMEM((NBR, slab // TILE), jnp.int32),
                pltpu.VMEM(table.shape, BF16),
                pltpu.VMEM((tiles, TILE, 2 * TILE), BF16),
                pltpu.VMEM((tiles, 2 * TILE, TILE), BF16),
                pltpu.VMEM((2, near, 16, TILE), F32),
                pltpu.VMEM((near, TILE, TILE), BF16),
                pltpu.VMEM((near, 32, TILE), BF16),
                pltpu.VMEM((tiles, TILE, KEPT * TILE), BF16),
                pltpu.SemaphoreType.DMA((10,)),
                pltpu.SemaphoreType.DMA((4,)),
                pltpu.SemaphoreType.DMA((4,)),
                pltpu.SemaphoreType.DMA((1 + tiles // CHUNK,)),
                pltpu.SemaphoreType.DMA((2,)),
                pltpu.SemaphoreType.DMA((2,)),
            ],
            compiler_params=pltpu.CompilerParams(collective_id=0, has_side_effects=True),
        )(
            jnp.transpose(positions, (1, 0, 2)),
            jnp.transpose(momenta, (1, 0, 2)),
            masses.reshape(-1, TILE),
            strengths.reshape(-1, TILE),
            bond_ends,
            angle_ends,
            neighbour_tiles,
            jnp.asarray(table),
        )
        done = [pltpu.with_memory_space_constraint(x, pltpu.VMEM) for x in done]
        plain = jax.ShapeDtypeStruct((3, held, slab), F32)
        done = pl.pallas_call(
            put_out,
            out_shape=(plain, plain),
            in_specs=[anywhere] * 2,
            out_specs=(anywhere, anywhere),
            scratch_shapes=[pltpu.SemaphoreType.DMA((2,))],
        )(*done)
        return tuple(jnp.transpose(x, (1, 0, 2)) for x in done)

    placed = (
        P("bead", None, "space"),
        P("bead", None, "space"),
        P("space"),
        P("space"),
        P(None, "space"),
        P(None, "space"),
        P(None, "space"),
    )
    return jax.shard_map(
        body,
        mesh=mesh,
        in_specs=placed,
        out_specs=(P("bead", None, "space"), P("bead", None, "space")),
        check_vma=False,
    )
```

```python
import functools
import math

import jax
import jax.numpy as jnp
import ml_dtypes
import numpy as np
from jax import lax
from jax.experimental import pallas as pl
from jax.experimental.pallas import tpu as pltpu
from jax.sharding import PartitionSpec as P

BEADS = 32
KEPT = 4
SUBS = 3
TILE = 128
GT = 2
NBR = 3
BPT = 128
APT = 64

time_step = 0.3
spring_freq = 80.0
bond_stiff = 0.2
bond_rest = 1.0
angle_stiff = 0.1
angle_rest = 0.5
range_sq = 4.0
CHUNK = 2

F32 = jnp.float32
BF16 = jnp.bfloat16
MESH = pl.DeviceIdType.MESH


def mode_table(number):
    within = np.arange(number)
    result = np.zeros((number, number))
    for column in range(number):
        if column == 0:
            result[:, column] = 1.0 / math.sqrt(number)
        elif 2 * column < number:
            result[:, column] = math.sqrt(2.0 / number) * np.cos(2 * np.pi * within * column / number)
        elif 2 * column == number:
            result[:, column] = (-1.0) ** within / math.sqrt(number)
        else:
            result[:, column] = math.sqrt(2.0 / number) * np.sin(2 * np.pi * within * column / number)
    return result


def contract_table(number, kept):
    larger = mode_table(number)
    smaller = mode_table(kept)
    chosen = [column if 2 * column <= kept else number - kept + column for column in range(kept)]
    return math.sqrt(kept / number) * smaller @ larger[:, chosen].T


def halves(table):
    high = table.astype(ml_dtypes.bfloat16)
    low = (table - high.astype(np.float64)).astype(ml_dtypes.bfloat16)
    return high, low


def three_products(table):
    high, low = halves(table)
    return np.concatenate([high, low, high], axis=1)


def stacked_rows(table):
    high, low = halves(table)
    return np.block([[high, high], [low, low]])


def constant_table():
    modes = mode_table(BEADS)
    interval = time_step / SUBS
    freqs = 2.0 * spring_freq * np.sin(np.pi * np.arange(BEADS) / BEADS)
    safe = np.where(freqs > 0, freqs, 1.0)
    cosine = np.cos(freqs * interval)
    gains = np.where(freqs > 0, np.sin(freqs * interval) / safe, interval)
    drags = freqs * np.sin(freqs * interval)
    keep = (modes * cosine) @ modes.T
    gain = (modes * gains) @ modes.T
    drag = -(modes * drags) @ modes.T
    free = np.block([[keep, gain], [drag, keep]])
    contract = contract_table(BEADS, KEPT)
    narrow = np.zeros((16, 3 * BEADS))
    for k in range(KEPT):
        for c in range(3):
            narrow[3 * k + c, c * BEADS : (c + 1) * BEADS] = contract[k]
    expand = BEADS / KEPT * contract.T
    wide = np.zeros((3 * BEADS, 16))
    for k in range(KEPT):
        for c in range(3):
            wide[c * BEADS : (c + 1) * BEADS, 3 * k + c] = expand[:, k]
    wide *= 0.5 * time_step * 2.0 / range_sq
    table = np.zeros((544, 256), ml_dtypes.bfloat16)
    table[:128, :128] = stacked_rows(free)
    for c in range(3):
        near = narrow[:, c * BEADS : (c + 1) * BEADS] @ free[:BEADS]
        table[128 + 32 * c : 160 + 32 * c, :128] = stacked_rows(near)
    table[224:256, :192] = stacked_rows(narrow)
    table[256:352, :48] = three_products(wide)
    kicked = [free[:, BEADS:] @ wide[c * BEADS : (c + 1) * BEADS] for c in range(3)]
    table[352:544, :48] = three_products(np.concatenate(kicked, axis=0))
    return table


def split2(x):
    high = x.astype(BF16)
    return high, (x - high.astype(F32)).astype(BF16)


def split3(x):
    high = x.astype(BF16)
    rest = x - high.astype(F32)
    middle = rest.astype(BF16)
    return high, middle, (rest - middle.astype(F32)).astype(BF16)


def mm(a, b):
    return jnp.dot(a, b, preferred_element_type=F32)


def lanes(x, t):
    return x[:, t * TILE : (t + 1) * TILE]


def walk(space, place, beads):
    core = lax.rem(space, 2)
    return core * (beads - 1) + (1 - 2 * core) * place


def flip(space):
    return 1 - lax.rem(lax.div(space, 2), 2)


def block_of(space, bead, beads):
    row = lax.div(bead, 2)
    return walk(space, 2 * row + lax.rem(bead + row + flip(space), 2), beads)


def device_of(spot, beads):
    space = lax.div(spot, beads)
    place = walk(space, lax.rem(spot, beads), beads)
    row = lax.div(place, 2)
    return space, 2 * row + lax.rem(place + row + flip(space), 2)


def kernel(
    spaces,
    beads,
    q_in,
    p_in,
    mass_in,
    strength_in,
    bond_in,
    angle_in,
    nbr_in,
    const_in,
    q_out,
    p_out,
    q_stage,
    p_stage,
    q_all,
    p_all,
    q_done,
    p_done,
    mass_v,
    strength_v,
    bond_v,
    angle_v,
    nbr_s,
    const_v,
    pick,
    drop,
    ext,
    a_side,
    g_side,
    own_side,
    local_sem,
    send_sem,
    recv_sem,
    own_sem,
    halo_send,
    halo_recv,
):
    space = lax.axis_index("space")
    me = lax.axis_index("bead")
    slab = q_in.shape[2]
    own = slab // beads
    tiles = own // TILE
    held = q_in.shape[1]
    total = spaces * beads
    block = block_of(space, me, beads)
    spot = space * beads + block
    after_id = device_of(lax.rem(spot + 1, total), beads)
    before_id = device_of(lax.rem(spot + total - 1, total), beads)
    peers = [lax.rem(me + d, beads) for d in range(1, beads)]
    order = sorted(range(beads - 1), key=lambda n: -min(n + 1, beads - n - 1))

    early = pltpu.make_async_copy(q_in, q_stage, local_sem.at[0])

    @pl.when(me >= 0)
    def _():
        early.start()

    barrier = pltpu.get_barrier_semaphore()
    for peer in peers:
        pl.semaphore_signal(barrier, inc=1, device_id=(space, peer), device_id_type=MESH)
    for device in (before_id, after_id):
        pl.semaphore_signal(barrier, inc=1, device_id=device, device_id_type=MESH)

    my_rows = pl.ds(pl.multiple_of(held * me, held), held)
    my_lanes = pl.ds(pl.multiple_of(own * block, own), own)
    local = [
        (q_in, q_stage),
        (p_in, p_stage),
        (q_in.at[:, :, my_lanes], q_all.at[:, my_rows, :]),
        (p_in.at[:, :, my_lanes], p_all.at[:, my_rows, :]),
        (bond_in.at[:, my_lanes], bond_v),
        (angle_in.at[:, pl.ds(pl.multiple_of((own // 2) * block, own // 2), own // 2)], angle_v),
        (mass_in, mass_v),
        (strength_in, strength_v),
        (nbr_in, nbr_s),
        (const_in, const_v),
    ]
    local = [pltpu.make_async_copy(a, b, local_sem.at[n]) for n, (a, b) in enumerate(local)]
    for copy in local[1:]:
        copy.start()

    def exchange(kind, source, target):
        for n in order:
            pltpu.make_async_remote_copy(
                src_ref=source(peers[n]),
                dst_ref=target,
                send_sem=send_sem.at[kind],
                recv_sem=recv_sem.at[kind],
                device_id=(space, peers[n]),
                device_id_type=MESH,
            ).start()

    def wait_all(sem):
        sized = q_stage.at[:, :, pl.ds(0, (beads - 1) * own)]
        pltpu.make_async_copy(sized, sized, sem).wait()

    def lanes_of(ref):
        return lambda peer: ref.at[:, :, pl.ds(pl.multiple_of(own * block_of(space, peer, beads), own), own)]

    def rows_of(ref):
        return lambda peer: ref.at[:, pl.ds(pl.multiple_of(held * peer, held), held), :]

    pl.semaphore_wait(barrier, beads + 1)
    local[0].wait()
    exchange(0, lanes_of(q_stage), q_all.at[:, my_rows, :])
    local[1].wait()
    exchange(1, lanes_of(p_stage), p_all.at[:, my_rows, :])

    for n in (4, 5, 6, 7, 8, 9):
        local[n].wait()

    place = lax.broadcasted_iota(jnp.int32, (TILE, TILE), 0)
    lane = lax.broadcasted_iota(jnp.int32, (8, TILE), 1)

    def hot(row):
        return jnp.where(place == row, 1.0, 0.0).astype(F32)

    for t in range(tiles):
        ends = bond_v[:, t * TILE : (t + 1) * TILE]
        bonds = hot(ends[0:1]) - hot(ends[1:2])
        pair = angle_v[:, (t // 2) * TILE : (t // 2 + 1) * TILE]
        rows = [jnp.broadcast_to(pair[e : e + 1], (8, TILE)) for e in range(3)]
        turned = [pltpu.roll(r, APT, 1) for r in rows]
        left, right = (rows, turned) if t % 2 == 0 else (turned, rows)
        outer = jnp.where(lane < APT, left[0], right[2])[0:1]
        centre = jnp.where(lane < APT, left[1], right[1])[0:1]
        angles = hot(outer) - hot(centre)
        pick[t] = jnp.concatenate([bonds, angles], axis=1).astype(BF16)
        drop[t] = jnp.concatenate([jnp.transpose(bonds), jnp.transpose(angles)], axis=0).astype(BF16)

    mass_row = jnp.concatenate([mass_v[pl.ds(tiles * block + t, 1), :] for t in range(tiles)], axis=1)
    inverse = 1.0 / mass_row
    strengths = [strength_v[pl.ds(tiles * block + t, 1), :] for t in range(tiles)]

    free_rows = const_v[0:128, 0:128]
    near_rows = [const_v[128 + 32 * c : 160 + 32 * c, 0:128] for c in range(3)]
    narrow_rows = const_v[224:256, 0:192]
    wide_table = const_v[256:352, 0:48]
    kick_table = const_v[352:544, 0:48]

    row16 = lax.broadcasted_iota(jnp.int32, (16, TILE), 0)
    feature = row16 < 12
    row_wide = lax.broadcasted_iota(jnp.int32, (16, own), 0)

    def contracted(current):
        high, low = split2(jnp.concatenate(current, axis=0))
        got = mm(narrow_rows, jnp.concatenate([high, low], axis=0))
        return got[:16] + got[16:]

    def start_halo(turn, narrow):
        for t in range(tiles):
            ext[turn, GT + t] = jnp.where(feature, lanes(narrow, t), strengths[t])
        for device, source, target in ((before_id, GT, GT + tiles), (after_id, tiles, 0)):
            pltpu.make_async_remote_copy(
                src_ref=ext.at[turn, pl.ds(source, GT)],
                dst_ref=ext.at[turn, pl.ds(target, GT)],
                send_sem=halo_send.at[turn],
                recv_sem=halo_recv.at[turn],
                device_id=device,
                device_id_type=MESH,
            ).start()

    def wait_halo(sem):
        both = ext.at[0, pl.ds(0, 2 * GT)]
        pltpu.make_async_copy(both, both, sem).wait()

    scale = math.sqrt(2.0 / range_sq * math.log2(math.e))

    def sides(turn, u, with_own):
        rows = ext[turn, u]
        scaled = rows * scale
        square = scaled * scaled
        norms = scaled
        for k in range(KEPT):
            part = 0.5 * (square[3 * k : 3 * k + 1] + square[3 * k + 1 : 3 * k + 2] + square[3 * k + 2 : 3 * k + 3])
            norms = jnp.where(row16 == 12 + k, part, norms)
        parts = split3(norms)
        wide_parts = [x.astype(F32) for x in parts]
        ones = [jnp.where(feature, x, 1.0) for x in wide_parts]
        stack = jnp.concatenate(
            [wide_parts[0], wide_parts[1], ones[0], ones[1], wide_parts[2], ones[0], jnp.zeros((32, TILE), F32)], axis=0
        )
        a_side[u] = jnp.transpose(stack).astype(BF16)
        weight = rows[12:13]
        g_high, g_low = split2(jnp.where(feature, rows * weight, weight))
        g_side[u] = jnp.concatenate([g_high, g_low], axis=0)
        if not with_own:
            return None
        h, m, l = wide_parts

        def own_block(left, right):
            return jnp.where(feature, left, right)

        minus = -jnp.ones_like(h)

        def shift(x):
            return -x

        full = [
            own_block(h, minus),
            own_block(h, minus),
            own_block(m, shift(h)),
            own_block(m, shift(m)),
            own_block(h, minus),
            own_block(l, shift(l)),
        ]
        return full

    def masks():
        found = []
        for k in range(KEPT):
            keep = (row16 >= 3 * k) & (row16 < 3 * k + 3) | (row16 == 12 + k)
            found.append(keep)
        return found

    kept_rows = masks()

    def prepare(turn):
        for t in range(tiles):
            full = sides(turn, GT + t, True)
            parts = []
            for k in range(KEPT):
                blocks = [jnp.where(kept_rows[k], x, 0.0) for x in full]
                parts.append(jnp.concatenate(blocks + [jnp.zeros((32, TILE), F32)], axis=0))
            own_side[t] = jnp.concatenate(parts, axis=1).astype(BF16)
        wait_halo(halo_recv.at[turn])
        for u in list(range(GT)) + list(range(GT + tiles, 2 * GT + tiles)):
            sides(turn, u, False)

    def nonbonded(turn, finish, chunk):
        base = spot * tiles - GT
        count = total * tiles
        found = []
        for t in range(tiles):
            near = [
                jnp.minimum(lax.rem(nbr_s[j, tiles * block + t] - base + count, count), tiles + 2 * GT - 1)
                for j in range(NBR)
            ]
            a = jnp.concatenate([a_side[u] for u in near], axis=0)
            g = [g_side[u] for u in near]
            g = jnp.concatenate([x for x in g for _ in range(2)], axis=1)
            rows = ext[turn, GT + t]
            weights = jnp.exp2(mm(a, own_side[t]))
            stack = []
            for j in range(NBR):
                stack.extend(split2(weights[j * TILE : (j + 1) * TILE]))
            got = mm(g, jnp.concatenate(stack, axis=0))
            got = got[0:16] + got[16:32]
            force = jnp.zeros((16, TILE), F32)
            for k in range(KEPT):
                both = lanes(got, k)
                force = jnp.where((row16 >= 3 * k) & (row16 < 3 * k + 3), rows * both[12:13] - both, force)
            found.append(force * strengths[t])
            if len(found) == chunk:
                finish(t, jnp.concatenate(found, axis=1))
                found = []

    def bonded(current, chosen):
        forces = []
        for n, t in enumerate(chosen):
            high, low = split2(jnp.concatenate([lanes(x, n) for x in current], axis=0))
            table = pick[t]
            got = mm(jnp.concatenate([high, low], axis=0), table)
            got = got[: 3 * BEADS] + got[3 * BEADS :]
            stretch = [got[c * BEADS : (c + 1) * BEADS, :TILE] for c in range(3)]
            arms = [got[c * BEADS : (c + 1) * BEADS, TILE:] for c in range(3)]
            swapped = [pltpu.roll(x, APT, 1) for x in arms]
            factor = -bond_stiff * (sum(x * x for x in stretch) - bond_rest)
            bend = -angle_stiff * (sum(x * y for x, y in zip(arms, swapped)) - angle_rest)
            push = jnp.concatenate(
                [jnp.concatenate([factor * x, bend * y], axis=1) for x, y in zip(stretch, swapped)], axis=0
            )
            high, low = split2(push)
            back = drop[t]
            got = mm(jnp.concatenate([high, low], axis=0), back)
            forces.append(got[: 3 * BEADS] + got[3 * BEADS :])
        return [
            jnp.concatenate([f[c * BEADS : (c + 1) * BEADS] for f in forces], axis=1) for c in range(3)
        ]

    def advance(current, speed, last=False):
        if not last:
            firsts = [x[0:1] for x in current]
            both = jnp.concatenate(
                [jnp.concatenate([x - f, y], axis=0) for x, f, y in zip(current, firsts, speed)], axis=1
            )
            high, low = split2(both)
            got = mm(free_rows, jnp.concatenate([high, low], axis=0))
            got = got[: 2 * BEADS] + got[2 * BEADS :]
            got = [got[:, c * own : (c + 1) * own] for c in range(3)]
            return [f + g[:BEADS] for f, g in zip(firsts, got)], [g[BEADS:] for g in got], None
        moved, fast = [], []
        narrow = None
        for c in range(3):
            first = current[c][0:1]
            both = jnp.concatenate([current[c] - first, speed[c]], axis=0)
            high, low = split2(both)
            table = jnp.concatenate([free_rows, near_rows[c]], axis=0) if last else free_rows
            got = mm(table, jnp.concatenate([high, low], axis=0))
            if last:
                part = got[4 * BEADS : 4 * BEADS + 16] + got[4 * BEADS + 16 :]
                part = part + jnp.where(lax.rem(row_wide, 3) == c, first, 0.0)
                narrow = part if narrow is None else narrow + part
            got = got[: 2 * BEADS] + got[2 * BEADS : 4 * BEADS]
            moved.append(first + got[:BEADS])
            fast.append(got[BEADS:])
        return moved, fast, narrow

    half = 0.5 * time_step / SUBS

    local[2].wait()
    wait_all(recv_sem.at[0])
    current = [q_all[c] for c in range(3)]
    start_halo(0, contracted(current))
    everything = list(range(tiles))
    pushed = bonded(current, everything)
    local[3].wait()
    wait_all(recv_sem.at[1])
    speed = [(p_all[c] + half * pushed[c]) * inverse for c in range(3)]
    current, speed, _ = advance(current, speed)
    found = []

    def keep(t, force):
        found.append(force)

    prepare(0)
    nonbonded(0, keep, tiles)
    high, low = split2(found[0] * inverse)
    shift = mm(kick_table, jnp.concatenate([high, high, low], axis=0))
    current = [x + shift[2 * BEADS * c : 2 * BEADS * c + BEADS] for c, x in enumerate(current)]
    speed = [x + shift[2 * BEADS * c + BEADS : 2 * BEADS * (c + 1)] for c, x in enumerate(speed)]
    for substep in range(1, SUBS):
        force = bonded(current, everything)
        speed = [speed[c] + (2.0 * half) * force[c] * inverse for c in range(3)]
        current, speed, narrow = advance(current, speed, substep == SUBS - 1)
    start_halo(1, narrow)
    for c in range(3):
        q_done[c] = current[c]
    exchange(2, rows_of(q_done), q_out.at[:, :, my_lanes])
    mine_q = pltpu.make_async_copy(q_done.at[:, my_rows, :], q_out.at[:, :, my_lanes], own_sem.at[0])
    mine_q.start()
    pushed = bonded(current, everything)
    moment = [speed[c] * mass_row + half * pushed[c] for c in range(3)]
    late = []

    def send_home(t, force):
        high, low = split2(force)
        kick = mm(wide_table, jnp.concatenate([high, high, low], axis=0))
        width = CHUNK * TILE
        begin = (t + 1 - CHUNK) * TILE
        for c in range(3):
            p_done[c, :, begin : begin + width] = (
                moment[c][:, begin : begin + width] + kick[c * BEADS : (c + 1) * BEADS]
            )
        here = pl.ds(pl.multiple_of(own * block + begin, TILE), width)
        target = p_out.at[:, :, here]
        for n in order:
            rows = pl.ds(pl.multiple_of(held * peers[n], held), held)
            pltpu.make_async_remote_copy(
                src_ref=p_done.at[:, rows, begin : begin + width],
                dst_ref=target,
                send_sem=send_sem.at[3],
                recv_sem=recv_sem.at[3],
                device_id=(space, peers[n]),
                device_id_type=MESH,
            ).start()
        mine = pltpu.make_async_copy(p_done.at[:, my_rows, begin : begin + width], target, own_sem.at[1 + t // CHUNK])
        mine.start()
        late.append(mine)

    prepare(1)
    nonbonded(1, send_home, CHUNK)
    for kind in range(4):
        wait_all(send_sem.at[kind])
    for turn in range(2):
        wait_halo(halo_send.at[turn])
    wait_all(recv_sem.at[2])
    mine_q.wait()
    for copy in late:
        copy.wait()
    wait_all(recv_sem.at[3])


def put_out(q_ref, p_ref, q_out, p_out, sem):
    copies = [
        pltpu.make_async_copy(a, b, sem.at[n]) for n, (a, b) in enumerate(((q_ref, q_out), (p_ref, p_out)))
    ]
    for copy in copies:
        copy.start()
    for copy in copies:
        copy.wait()


def solution(mesh):
    spaces, beads = mesh.shape["space"], mesh.shape["bead"]
    table = constant_table()

    def body(positions, momenta, masses, strengths, bond_ends, angle_ends, neighbour_tiles):
        held, _, slab = positions.shape
        own = slab // beads
        tiles = own // TILE
        near = tiles + 2 * GT
        moved = pltpu.VMEM((3, held, slab), F32)
        anywhere = pl.BlockSpec(memory_space=pl.ANY)
        done = pl.pallas_call(
            functools.partial(kernel, spaces, beads),
            out_shape=(moved, moved),
            in_specs=[anywhere] * 8,
            out_specs=(pl.BlockSpec(memory_space=pltpu.VMEM),) * 2,
            scratch_shapes=[
                pltpu.VMEM((3, held, slab), F32),
                pltpu.VMEM((3, held, slab), F32),
                pltpu.VMEM((3, BEADS, own), F32),
                pltpu.VMEM((3, BEADS, own), F32),
                pltpu.VMEM((3, BEADS, own), F32),
                pltpu.VMEM((3, BEADS, own), F32),
                pltpu.VMEM((slab // TILE, TILE), F32),
                pltpu.VMEM((slab // TILE, TILE), F32),
                pltpu.VMEM((2, own), jnp.int32),
                pltpu.VMEM((3, own // 2), jnp.int32),
                pltpu.SMEM((NBR, slab // TILE), jnp.int32),
                pltpu.VMEM(table.shape, BF16),
                pltpu.VMEM((tiles, TILE, 2 * TILE), BF16),
                pltpu.VMEM((tiles, 2 * TILE, TILE), BF16),
                pltpu.VMEM((2, near, 16, TILE), F32),
                pltpu.VMEM((near, TILE, TILE), BF16),
                pltpu.VMEM((near, 32, TILE), BF16),
                pltpu.VMEM((tiles, TILE, KEPT * TILE), BF16),
                pltpu.SemaphoreType.DMA((10,)),
                pltpu.SemaphoreType.DMA((4,)),
                pltpu.SemaphoreType.DMA((4,)),
                pltpu.SemaphoreType.DMA((1 + tiles // CHUNK,)),
                pltpu.SemaphoreType.DMA((2,)),
                pltpu.SemaphoreType.DMA((2,)),
            ],
            compiler_params=pltpu.CompilerParams(collective_id=0, has_side_effects=True),
        )(
            jnp.transpose(positions, (1, 0, 2)),
            jnp.transpose(momenta, (1, 0, 2)),
            masses.reshape(-1, TILE),
            strengths.reshape(-1, TILE),
            bond_ends,
            angle_ends,
            neighbour_tiles,
            jnp.asarray(table),
        )
        done = [pltpu.with_memory_space_constraint(x, pltpu.VMEM) for x in done]
        plain = jax.ShapeDtypeStruct((3, held, slab), F32)
        done = pl.pallas_call(
            put_out,
            out_shape=(plain, plain),
            in_specs=[anywhere] * 2,
            out_specs=(anywhere, anywhere),
            scratch_shapes=[pltpu.SemaphoreType.DMA((2,))],
        )(*done)
        return tuple(jnp.transpose(x, (1, 0, 2)) for x in done)

    placed = (
        P("bead", None, "space"),
        P("bead", None, "space"),
        P("space"),
        P("space"),
        P(None, "space"),
        P(None, "space"),
        P(None, "space"),
    )
    return jax.shard_map(
        body,
        mesh=mesh,
        in_specs=placed,
        out_specs=(P("bead", None, "space"), P("bead", None, "space")),
        check_vma=False,
    )
```

```python
import functools
import math

import jax
import jax.numpy as jnp
import ml_dtypes
import numpy as np
from jax import lax
from jax.experimental import pallas as pl
from jax.experimental.pallas import tpu as pltpu
from jax.sharding import PartitionSpec as P

BEADS = 32
KEPT = 4
SUBS = 3
TILE = 128
GT = 2
NBR = 3
BPT = 128
APT = 64

time_step = 0.3
spring_freq = 80.0
bond_stiff = 0.2
bond_rest = 1.0
angle_stiff = 0.1
angle_rest = 0.5
range_sq = 4.0

F32 = jnp.float32
BF16 = jnp.bfloat16
MESH = pl.DeviceIdType.MESH


def mode_table(number):
    within = np.arange(number)
    result = np.zeros((number, number))
    for column in range(number):
        if column == 0:
            result[:, column] = 1.0 / math.sqrt(number)
        elif 2 * column < number:
            result[:, column] = math.sqrt(2.0 / number) * np.cos(2 * np.pi * within * column / number)
        elif 2 * column == number:
            result[:, column] = (-1.0) ** within / math.sqrt(number)
        else:
            result[:, column] = math.sqrt(2.0 / number) * np.sin(2 * np.pi * within * column / number)
    return result


def contract_table(number, kept):
    larger = mode_table(number)
    smaller = mode_table(kept)
    chosen = [column if 2 * column <= kept else number - kept + column for column in range(kept)]
    return math.sqrt(kept / number) * smaller @ larger[:, chosen].T


def halves(table):
    high = table.astype(ml_dtypes.bfloat16)
    low = (table - high.astype(np.float64)).astype(ml_dtypes.bfloat16)
    return high, low


def three_products(table):
    high, low = halves(table)
    return np.concatenate([high, low, high], axis=1)


def stacked_rows(table):
    high, low = halves(table)
    return np.block([[high, high], [low, low]])


def constant_table():
    modes = mode_table(BEADS)
    interval = time_step / SUBS
    freqs = 2.0 * spring_freq * np.sin(np.pi * np.arange(BEADS) / BEADS)
    safe = np.where(freqs > 0, freqs, 1.0)
    cosine = np.cos(freqs * interval)
    gains = np.where(freqs > 0, np.sin(freqs * interval) / safe, interval)
    drags = freqs * np.sin(freqs * interval)
    keep = (modes * cosine) @ modes.T
    gain = (modes * gains) @ modes.T
    drag = -(modes * drags) @ modes.T
    free = np.block([[keep, gain], [drag, keep]])
    contract = contract_table(BEADS, KEPT)
    narrow = np.zeros((16, 3 * BEADS))
    for k in range(KEPT):
        for c in range(3):
            narrow[3 * k + c, c * BEADS : (c + 1) * BEADS] = contract[k]
    expand = BEADS / KEPT * contract.T
    wide = np.zeros((3 * BEADS, 16))
    for k in range(KEPT):
        for c in range(3):
            wide[c * BEADS : (c + 1) * BEADS, 3 * k + c] = expand[:, k]
    wide *= 0.5 * time_step * 2.0 / range_sq
    table = np.zeros((544, 256), ml_dtypes.bfloat16)
    table[:128, :128] = stacked_rows(free)
    for c in range(3):
        near = narrow[:, c * BEADS : (c + 1) * BEADS] @ free[:BEADS]
        table[128 + 32 * c : 160 + 32 * c, :128] = stacked_rows(near)
    table[224:256, :192] = stacked_rows(narrow)
    table[256:352, :48] = three_products(wide)
    kicked = [free[:, BEADS:] @ wide[c * BEADS : (c + 1) * BEADS] for c in range(3)]
    table[352:544, :48] = three_products(np.concatenate(kicked, axis=0))
    return table


def split2(x):
    high = x.astype(BF16)
    return high, (x - high.astype(F32)).astype(BF16)


def split3(x):
    high = x.astype(BF16)
    rest = x - high.astype(F32)
    middle = rest.astype(BF16)
    return high, middle, (rest - middle.astype(F32)).astype(BF16)


def mm(a, b):
    return jnp.dot(a, b, preferred_element_type=F32)


def lanes(x, t):
    return x[:, t * TILE : (t + 1) * TILE]


def walk(space, place, beads):
    core = lax.rem(space, 2)
    return core * (beads - 1) + (1 - 2 * core) * place


def flip(space):
    return 1 - lax.rem(lax.div(space, 2), 2)


def block_of(space, bead, beads):
    row = lax.div(bead, 2)
    return walk(space, 2 * row + lax.rem(bead + row + flip(space), 2), beads)


def device_of(spot, beads):
    space = lax.div(spot, beads)
    place = walk(space, lax.rem(spot, beads), beads)
    row = lax.div(place, 2)
    return space, 2 * row + lax.rem(place + row + flip(space), 2)


def kernel(
    spaces,
    beads,
    q_in,
    p_in,
    mass_in,
    strength_in,
    bond_in,
    angle_in,
    nbr_in,
    const_in,
    q_out,
    p_out,
    q_stage,
    p_stage,
    q_all,
    p_all,
    q_done,
    p_done,
    mass_v,
    strength_v,
    bond_v,
    angle_v,
    nbr_s,
    const_v,
    pick,
    drop,
    ext,
    a_side,
    g_side,
    own_side,
    local_sem,
    send_sem,
    recv_sem,
    own_sem,
    halo_send,
    halo_recv,
):
    space = lax.axis_index("space")
    me = lax.axis_index("bead")
    slab = q_in.shape[2]
    own = slab // beads
    tiles = own // TILE
    held = q_in.shape[1]
    total = spaces * beads
    block = block_of(space, me, beads)
    spot = space * beads + block
    after_id = device_of(lax.rem(spot + 1, total), beads)
    before_id = device_of(lax.rem(spot + total - 1, total), beads)
    peers = [lax.rem(me + d, beads) for d in range(1, beads)]
    order = sorted(range(beads - 1), key=lambda n: -min(n + 1, beads - n - 1))

    early = pltpu.make_async_copy(q_in, q_stage, local_sem.at[0])

    @pl.when(me >= 0)
    def _():
        early.start()

    barrier = pltpu.get_barrier_semaphore()
    for peer in peers:
        pl.semaphore_signal(barrier, inc=1, device_id=(space, peer), device_id_type=MESH)
    for device in (before_id, after_id):
        pl.semaphore_signal(barrier, inc=1, device_id=device, device_id_type=MESH)

    my_rows = pl.ds(pl.multiple_of(held * me, held), held)
    my_lanes = pl.ds(pl.multiple_of(own * block, own), own)
    local = [
        (q_in, q_stage),
        (p_in, p_stage),
        (q_in.at[:, :, my_lanes], q_all.at[:, my_rows, :]),
        (p_in.at[:, :, my_lanes], p_all.at[:, my_rows, :]),
        (bond_in.at[:, my_lanes], bond_v),
        (angle_in.at[:, pl.ds(pl.multiple_of((own // 2) * block, own // 2), own // 2)], angle_v),
        (mass_in, mass_v),
        (strength_in, strength_v),
        (nbr_in, nbr_s),
        (const_in, const_v),
    ]
    local = [pltpu.make_async_copy(a, b, local_sem.at[n]) for n, (a, b) in enumerate(local)]
    for copy in local[1:]:
        copy.start()

    def exchange(kind, source, target):
        for n in order:
            pltpu.make_async_remote_copy(
                src_ref=source(peers[n]),
                dst_ref=target,
                send_sem=send_sem.at[kind],
                recv_sem=recv_sem.at[kind],
                device_id=(space, peers[n]),
                device_id_type=MESH,
            ).start()

    def wait_all(sem):
        sized = q_stage.at[:, :, pl.ds(0, (beads - 1) * own)]
        pltpu.make_async_copy(sized, sized, sem).wait()

    def lanes_of(ref):
        return lambda peer: ref.at[:, :, pl.ds(pl.multiple_of(own * block_of(space, peer, beads), own), own)]

    def rows_of(ref):
        return lambda peer: ref.at[:, pl.ds(pl.multiple_of(held * peer, held), held), :]

    pl.semaphore_wait(barrier, beads + 1)
    local[0].wait()
    exchange(0, lanes_of(q_stage), q_all.at[:, my_rows, :])
    local[1].wait()
    exchange(1, lanes_of(p_stage), p_all.at[:, my_rows, :])

    for n in (4, 5, 6, 7, 8, 9):
        local[n].wait()

    place = lax.broadcasted_iota(jnp.int32, (TILE, TILE), 0)
    lane = lax.broadcasted_iota(jnp.int32, (8, TILE), 1)

    def hot(row):
        return jnp.where(place == row, 1.0, 0.0).astype(F32)

    for t in range(tiles):
        ends = bond_v[:, t * TILE : (t + 1) * TILE]
        bonds = hot(ends[0:1]) - hot(ends[1:2])
        pair = angle_v[:, (t // 2) * TILE : (t // 2 + 1) * TILE]
        rows = [jnp.broadcast_to(pair[e : e + 1], (8, TILE)) for e in range(3)]
        turned = [pltpu.roll(r, APT, 1) for r in rows]
        left, right = (rows, turned) if t % 2 == 0 else (turned, rows)
        outer = jnp.where(lane < APT, left[0], right[2])[0:1]
        centre = jnp.where(lane < APT, left[1], right[1])[0:1]
        angles = hot(outer) - hot(centre)
        pick[t] = jnp.concatenate([bonds, angles], axis=1).astype(BF16)
        drop[t] = jnp.concatenate([jnp.transpose(bonds), jnp.transpose(angles)], axis=0).astype(BF16)

    mass_row = jnp.concatenate([mass_v[pl.ds(tiles * block + t, 1), :] for t in range(tiles)], axis=1)
    inverse = 1.0 / mass_row
    strengths = [strength_v[pl.ds(tiles * block + t, 1), :] for t in range(tiles)]

    free_rows = const_v[0:128, 0:128]
    near_rows = [const_v[128 + 32 * c : 160 + 32 * c, 0:128] for c in range(3)]
    narrow_rows = const_v[224:256, 0:192]
    wide_table = const_v[256:352, 0:48]
    kick_table = const_v[352:544, 0:48]

    row16 = lax.broadcasted_iota(jnp.int32, (16, TILE), 0)
    feature = row16 < 12
    row_wide = lax.broadcasted_iota(jnp.int32, (16, own), 0)

    def contracted(current):
        high, low = split2(jnp.concatenate(current, axis=0))
        got = mm(narrow_rows, jnp.concatenate([high, low], axis=0))
        return got[:16] + got[16:]

    def start_halo(turn, narrow):
        for t in range(tiles):
            ext[turn, GT + t] = jnp.where(feature, lanes(narrow, t), strengths[t])
        for device, source, target in ((before_id, GT, GT + tiles), (after_id, tiles, 0)):
            pltpu.make_async_remote_copy(
                src_ref=ext.at[turn, pl.ds(source, GT)],
                dst_ref=ext.at[turn, pl.ds(target, GT)],
                send_sem=halo_send.at[turn],
                recv_sem=halo_recv.at[turn],
                device_id=device,
                device_id_type=MESH,
            ).start()

    def wait_halo(sem):
        both = ext.at[0, pl.ds(0, 2 * GT)]
        pltpu.make_async_copy(both, both, sem).wait()

    scale = math.sqrt(2.0 / range_sq * math.log2(math.e))

    def sides(turn, u, with_own):
        rows = ext[turn, u]
        scaled = rows * scale
        square = scaled * scaled
        norms = scaled
        for k in range(KEPT):
            part = 0.5 * (square[3 * k : 3 * k + 1] + square[3 * k + 1 : 3 * k + 2] + square[3 * k + 2 : 3 * k + 3])
            norms = jnp.where(row16 == 12 + k, part, norms)
        parts = split3(norms)
        wide_parts = [x.astype(F32) for x in parts]
        ones = [jnp.where(feature, x, 1.0) for x in wide_parts]
        stack = jnp.concatenate(
            [wide_parts[0], wide_parts[1], ones[0], ones[1], wide_parts[2], ones[0], jnp.zeros((32, TILE), F32)], axis=0
        )
        a_side[u] = jnp.transpose(stack).astype(BF16)
        weight = rows[12:13]
        g_high, g_low = split2(jnp.where(feature, rows * weight, weight))
        g_side[u] = jnp.concatenate([g_high, g_low], axis=0)
        if not with_own:
            return None
        h, m, l = wide_parts

        def own_block(left, right):
            return jnp.where(feature, left, right)

        minus = -jnp.ones_like(h)

        def shift(x):
            return -x

        full = [
            own_block(h, minus),
            own_block(h, minus),
            own_block(m, shift(h)),
            own_block(m, shift(m)),
            own_block(h, minus),
            own_block(l, shift(l)),
        ]
        return full

    def masks():
        found = []
        for k in range(KEPT):
            keep = (row16 >= 3 * k) & (row16 < 3 * k + 3) | (row16 == 12 + k)
            found.append(keep)
        return found

    kept_rows = masks()

    def prepare(turn):
        for t in range(tiles):
            full = sides(turn, GT + t, True)
            parts = []
            for k in range(KEPT):
                blocks = [jnp.where(kept_rows[k], x, 0.0) for x in full]
                parts.append(jnp.concatenate(blocks + [jnp.zeros((32, TILE), F32)], axis=0))
            own_side[t] = jnp.concatenate(parts, axis=1).astype(BF16)
        wait_halo(halo_recv.at[turn])
        for u in list(range(GT)) + list(range(GT + tiles, 2 * GT + tiles)):
            sides(turn, u, False)

    def nonbonded(turn, finish, ends):
        base = spot * tiles - GT
        count = total * tiles
        found = []
        for t in range(tiles):
            near = [
                jnp.minimum(lax.rem(nbr_s[j, tiles * block + t] - base + count, count), tiles + 2 * GT - 1)
                for j in range(NBR)
            ]
            a = jnp.concatenate([a_side[u] for u in near], axis=0)
            g = [g_side[u] for u in near]
            g = jnp.concatenate([x for x in g for _ in range(2)], axis=1)
            rows = ext[turn, GT + t]
            weights = jnp.exp2(mm(a, own_side[t]))
            stack = []
            for j in range(NBR):
                stack.extend(split2(weights[j * TILE : (j + 1) * TILE]))
            got = mm(g, jnp.concatenate(stack, axis=0))
            got = got[0:16] + got[16:32]
            force = jnp.zeros((16, TILE), F32)
            for k in range(KEPT):
                both = lanes(got, k)
                force = jnp.where((row16 >= 3 * k) & (row16 < 3 * k + 3), rows * both[12:13] - both, force)
            found.append(force * strengths[t])
            if t + 1 in ends:
                finish(t, jnp.concatenate(found, axis=1))
                found = []

    def bonded(current, chosen):
        forces = []
        for n, t in enumerate(chosen):
            high, low = split2(jnp.concatenate([lanes(x, n) for x in current], axis=0))
            table = pick[t]
            got = mm(jnp.concatenate([high, low], axis=0), table)
            got = got[: 3 * BEADS] + got[3 * BEADS :]
            stretch = [got[c * BEADS : (c + 1) * BEADS, :TILE] for c in range(3)]
            arms = [got[c * BEADS : (c + 1) * BEADS, TILE:] for c in range(3)]
            swapped = [pltpu.roll(x, APT, 1) for x in arms]
            factor = -bond_stiff * (sum(x * x for x in stretch) - bond_rest)
            bend = -angle_stiff * (sum(x * y for x, y in zip(arms, swapped)) - angle_rest)
            push = jnp.concatenate(
                [jnp.concatenate([factor * x, bend * y], axis=1) for x, y in zip(stretch, swapped)], axis=0
            )
            high, low = split2(push)
            back = drop[t]
            got = mm(jnp.concatenate([high, low], axis=0), back)
            forces.append(got[: 3 * BEADS] + got[3 * BEADS :])
        return [
            jnp.concatenate([f[c * BEADS : (c + 1) * BEADS] for f in forces], axis=1) for c in range(3)
        ]

    def advance(current, speed, last=False):
        if not last:
            firsts = [x[0:1] for x in current]
            both = jnp.concatenate(
                [jnp.concatenate([x - f, y], axis=0) for x, f, y in zip(current, firsts, speed)], axis=1
            )
            high, low = split2(both)
            got = mm(free_rows, jnp.concatenate([high, low], axis=0))
            got = got[: 2 * BEADS] + got[2 * BEADS :]
            got = [got[:, c * own : (c + 1) * own] for c in range(3)]
            return [f + g[:BEADS] for f, g in zip(firsts, got)], [g[BEADS:] for g in got], None
        moved, fast = [], []
        narrow = None
        for c in range(3):
            first = current[c][0:1]
            both = jnp.concatenate([current[c] - first, speed[c]], axis=0)
            high, low = split2(both)
            table = jnp.concatenate([free_rows, near_rows[c]], axis=0) if last else free_rows
            got = mm(table, jnp.concatenate([high, low], axis=0))
            if last:
                part = got[4 * BEADS : 4 * BEADS + 16] + got[4 * BEADS + 16 :]
                part = part + jnp.where(lax.rem(row_wide, 3) == c, first, 0.0)
                narrow = part if narrow is None else narrow + part
            got = got[: 2 * BEADS] + got[2 * BEADS : 4 * BEADS]
            moved.append(first + got[:BEADS])
            fast.append(got[BEADS:])
        return moved, fast, narrow

    half = 0.5 * time_step / SUBS

    local[2].wait()
    wait_all(recv_sem.at[0])
    current = [q_all[c] for c in range(3)]
    start_halo(0, contracted(current))
    everything = list(range(tiles))
    pushed = bonded(current, everything)
    local[3].wait()
    wait_all(recv_sem.at[1])
    speed = [(p_all[c] + half * pushed[c]) * inverse for c in range(3)]
    current, speed, _ = advance(current, speed)
    found = []

    def keep(t, force):
        found.append(force)

    prepare(0)
    nonbonded(0, keep, (tiles,))
    high, low = split2(found[0] * inverse)
    shift = mm(kick_table, jnp.concatenate([high, high, low], axis=0))
    current = [x + shift[2 * BEADS * c : 2 * BEADS * c + BEADS] for c, x in enumerate(current)]
    speed = [x + shift[2 * BEADS * c + BEADS : 2 * BEADS * (c + 1)] for c, x in enumerate(speed)]
    for substep in range(1, SUBS):
        force = bonded(current, everything)
        speed = [speed[c] + (2.0 * half) * force[c] * inverse for c in range(3)]
        current, speed, narrow = advance(current, speed, substep == SUBS - 1)
    start_halo(1, narrow)
    for c in range(3):
        q_done[c] = current[c]
    exchange(2, rows_of(q_done), q_out.at[:, :, my_lanes])
    mine_q = pltpu.make_async_copy(q_done.at[:, my_rows, :], q_out.at[:, :, my_lanes], own_sem.at[0])
    mine_q.start()
    pushed = bonded(current, everything)
    moment = [speed[c] * mass_row + half * pushed[c] for c in range(3)]
    late = []

    def send_home(t, force):
        high, low = split2(force)
        kick = mm(wide_table, jnp.concatenate([high, high, low], axis=0))
        width = force.shape[1]
        begin = (t + 1) * TILE - width
        for c in range(3):
            p_done[c, :, begin : begin + width] = (
                moment[c][:, begin : begin + width] + kick[c * BEADS : (c + 1) * BEADS]
            )
        here = pl.ds(pl.multiple_of(own * block + begin, TILE), width)
        target = p_out.at[:, :, here]
        for n in order:
            rows = pl.ds(pl.multiple_of(held * peers[n], held), held)
            pltpu.make_async_remote_copy(
                src_ref=p_done.at[:, rows, begin : begin + width],
                dst_ref=target,
                send_sem=send_sem.at[3],
                recv_sem=recv_sem.at[3],
                device_id=(space, peers[n]),
                device_id_type=MESH,
            ).start()
        mine = pltpu.make_async_copy(p_done.at[:, my_rows, begin : begin + width], target, own_sem.at[t + 3 - tiles])
        mine.start()
        late.append(mine)

    prepare(1)
    nonbonded(1, send_home, (tiles - 1, tiles))
    for kind in range(4):
        wait_all(send_sem.at[kind])
    for turn in range(2):
        wait_halo(halo_send.at[turn])
    wait_all(recv_sem.at[2])
    mine_q.wait()
    for copy in late:
        copy.wait()
    wait_all(recv_sem.at[3])


def put_out(q_ref, p_ref, q_out, p_out, sem):
    copies = [
        pltpu.make_async_copy(a, b, sem.at[n]) for n, (a, b) in enumerate(((q_ref, q_out), (p_ref, p_out)))
    ]
    for copy in copies:
        copy.start()
    for copy in copies:
        copy.wait()


def solution(mesh):
    spaces, beads = mesh.shape["space"], mesh.shape["bead"]
    table = constant_table()

    def body(positions, momenta, masses, strengths, bond_ends, angle_ends, neighbour_tiles):
        held, _, slab = positions.shape
        own = slab // beads
        tiles = own // TILE
        near = tiles + 2 * GT
        moved = pltpu.VMEM((3, held, slab), F32)
        anywhere = pl.BlockSpec(memory_space=pl.ANY)
        done = pl.pallas_call(
            functools.partial(kernel, spaces, beads),
            out_shape=(moved, moved),
            in_specs=[anywhere] * 8,
            out_specs=(pl.BlockSpec(memory_space=pltpu.VMEM),) * 2,
            scratch_shapes=[
                pltpu.VMEM((3, held, slab), F32),
                pltpu.VMEM((3, held, slab), F32),
                pltpu.VMEM((3, BEADS, own), F32),
                pltpu.VMEM((3, BEADS, own), F32),
                pltpu.VMEM((3, BEADS, own), F32),
                pltpu.VMEM((3, BEADS, own), F32),
                pltpu.VMEM((slab // TILE, TILE), F32),
                pltpu.VMEM((slab // TILE, TILE), F32),
                pltpu.VMEM((2, own), jnp.int32),
                pltpu.VMEM((3, own // 2), jnp.int32),
                pltpu.SMEM((NBR, slab // TILE), jnp.int32),
                pltpu.VMEM(table.shape, BF16),
                pltpu.VMEM((tiles, TILE, 2 * TILE), BF16),
                pltpu.VMEM((tiles, 2 * TILE, TILE), BF16),
                pltpu.VMEM((2, near, 16, TILE), F32),
                pltpu.VMEM((near, TILE, TILE), BF16),
                pltpu.VMEM((near, 32, TILE), BF16),
                pltpu.VMEM((tiles, TILE, KEPT * TILE), BF16),
                pltpu.SemaphoreType.DMA((10,)),
                pltpu.SemaphoreType.DMA((4,)),
                pltpu.SemaphoreType.DMA((4,)),
                pltpu.SemaphoreType.DMA((3,)),
                pltpu.SemaphoreType.DMA((2,)),
                pltpu.SemaphoreType.DMA((2,)),
            ],
            compiler_params=pltpu.CompilerParams(collective_id=0, has_side_effects=True),
        )(
            jnp.transpose(positions, (1, 0, 2)),
            jnp.transpose(momenta, (1, 0, 2)),
            masses.reshape(-1, TILE),
            strengths.reshape(-1, TILE),
            bond_ends,
            angle_ends,
            neighbour_tiles,
            jnp.asarray(table),
        )
        done = [pltpu.with_memory_space_constraint(x, pltpu.VMEM) for x in done]
        plain = jax.ShapeDtypeStruct((3, held, slab), F32)
        done = pl.pallas_call(
            put_out,
            out_shape=(plain, plain),
            in_specs=[anywhere] * 2,
            out_specs=(anywhere, anywhere),
            scratch_shapes=[pltpu.SemaphoreType.DMA((2,))],
        )(*done)
        return tuple(jnp.transpose(x, (1, 0, 2)) for x in done)

    placed = (
        P("bead", None, "space"),
        P("bead", None, "space"),
        P("space"),
        P("space"),
        P(None, "space"),
        P(None, "space"),
        P(None, "space"),
    )
    return jax.shard_map(
        body,
        mesh=mesh,
        in_specs=placed,
        out_specs=(P("bead", None, "space"), P("bead", None, "space")),
        check_vma=False,
    )
```
